512 devices in a mesh: side: 2 (over core), grp: 64 (over x, y, z_lo), head: 4 (over z_hi).
Axes of the slice: x: 4, y: 8, z: 8 (z_hi: 4, z_lo: 2; z = z_hi * 2 + z_lo), core: 2. Of those that a mesh axis runs over, the one named last changes fastest.
Arguments:
- q_new: bfloat16 [128, 64, 4096], P(('side', 'grp'), None, 'head'), may hold values from -12 to 12
- k_cache: bfloat16 [128, 4, 512, 128], P(('side', 'grp'), 'head'), may hold values from -12 to 12
- value_cache: bfloat16 [128, 4, 512, 128], P(('side', 'grp'), 'head'), may hold values from -12 to 12
- k_new: bfloat16 [128, 64, 512], P(('side', 'grp'), None, 'head'), may hold values from -12 to 12
- new_value_rows: bfloat16 [128, 64, 512], P(('side', 'grp'), None, 'head'), may hold values from -12 to 12
- cache_len: int32 [128], P(('side', 'grp')), may hold values from 1 to 512, 32768 in all
- hidden_in: bfloat16 [128, 64, 2048], P(('side', 'grp'), 'head'), may hold values from -8 to 8
- out_proj: bfloat16 [4096, 2048], P('head', 'side'), may hold values from -0.09375 to 0.09375
- norm_gain: float32 [2048], replicated, may hold values from 0.1 to 1.9
- expert_ids: int32 [128, 64, 8], P(('side', 'grp'), 'head'), may hold values from 0 to 127, all different within a row; in each aligned block of 16 rows (0 to 15, 16 to 31, ..., all dimensions but the last counted through in order) at most 2 rows name the same one
- gate_wts: float32 [128, 64, 8], P(('side', 'grp'), 'head'), may hold values from 0.05 to 1
- w_gate: bfloat16 [128, 2048, 768], P(('side', 'grp'), None, 'head'), may hold values from -0.125 to 0.125
- w_up: bfloat16 [128, 2048, 768], P(('side', 'grp'), None, 'head'), may hold values from -0.125 to 0.125
- w_down: bfloat16 [128, 768, 2048], P(('side', 'grp'), 'head'), may hold values from -0.21875 to 0.21875
Outputs:
- layer_out: bfloat16 [128, 64, 2048], P(('side', 'grp'), 'head')
The draws below stay inside these ranges and needn't reach their ends.
Inputs may be any that keep to these rules, and one draw needn't show every extreme that they name: `expert_ids`: each row names 8 different experts. In each aligned block of 16 rows (one stream's rows taken 16 at a time) no expert is named by more than 2 rows, a bound that some block reaches. `cache_len`: some stream has all 512 positions valid.
All inputs are finite; a program needn't handle non-finite values. No bound on the sum of `cache_len` on one device may be relied on, other than what follows from the above.
Results may differ from the reference program's by a relative error of at most 0.015.
Values may be sent and summed in bfloat16 or wider, within the bound.
No kernel may reach another device: no remote copies, remote signals or barrier semaphores. Data moves between devices by JAX's collectives and lax.ppermute only.
A program may use at most 64 MiB of HBM per device.

```python
import math
import jax
import jax.numpy as jnp
import numpy as np
from jax import lax

D = 2048
QUERY_HEADS = 32
KEY_VALUE_HEADS = 4
HEAD_SIZE = 128
FF = 768
TOPK = 8
NEW_TOKEN_ROWS = 64
CACHE_POSITIONS = 512
STREAM_COUNT = 128
EXPERTS = 128
ROWB = 16
FF_PART = 192
MOST = 2
N_HEAD = 4


def attention_parts(key):
    key_q, random_key_cache, random_key_normal = jax.random.split(jax.random.fold_in(key, 7), 3)
    query_rows = jnp.clip(jax.random.normal(key_q, (STREAM_COUNT, NEW_TOKEN_ROWS, QUERY_HEADS * HEAD_SIZE), jnp.float32), -6.0, 6.0)
    cached_part = jnp.clip(jax.random.normal(random_key_cache, (STREAM_COUNT, KEY_VALUE_HEADS, CACHE_POSITIONS, HEAD_SIZE), jnp.float32), -6.0, 6.0)
    fresh_part = jnp.clip(jax.random.normal(random_key_normal, (STREAM_COUNT, NEW_TOKEN_ROWS, KEY_VALUE_HEADS, HEAD_SIZE), jnp.float32), -6.0, 6.0)
    return (query_rows, cached_part, fresh_part.reshape(STREAM_COUNT, NEW_TOKEN_ROWS, KEY_VALUE_HEADS * HEAD_SIZE))


def draw_q_new(key, part):
    return attention_parts(key)[0].astype(jnp.bfloat16)


def draw_k_cache(key, part):
    return attention_parts(key)[1].astype(jnp.bfloat16)


def draw_k_new(key, part):
    return attention_parts(key)[2].astype(jnp.bfloat16)


def draw_hidden_in(key, part):
    key_r, random_key_cache, key_z = jax.random.split(jax.random.fold_in(key, 11), 3)
    row_scale = jnp.exp(jax.random.uniform(key_r, (STREAM_COUNT, NEW_TOKEN_ROWS, 1), jnp.float32, math.log(0.1), 0.0))
    col_scale = jnp.exp(jax.random.uniform(random_key_cache, (D,), jnp.float32, math.log(0.1), 0.0))
    base = jnp.clip(jax.random.normal(key_z, (STREAM_COUNT, NEW_TOKEN_ROWS, D), jnp.float32), -6.0, 6.0)
    return jnp.clip(base * row_scale * col_scale, -8.0, 8.0).astype(jnp.bfloat16)


def shard_levels(own_key, shape, cuts, smallest, top_value):
    factor_of = 1.0
    for position, blocks in cuts:
        draws = jax.random.uniform(jax.random.fold_in(jax.random.fold_in(own_key, 6), position), (blocks,), jnp.float32, smallest / len(cuts), top_value / len(cuts))
        factor_of = factor_of * jnp.repeat(jnp.exp(draws), shape[position] // blocks).reshape((-1,) + (1,) * (len(shape) - 1 - position))
    return factor_of


def length_profile(count, total, reach, lean):
    portions = [(1 << 20) // math.isqrt(standing ** lean) + 1 for standing in range(2, count + 1)]
    spare, counts = total - reach - (count - 1), [1] * (count - 1)
    while spare > 0:
        candidates = [i for i in range(count - 1) if counts[i] < reach]
        mass, budget = sum([portions[i] for i in candidates]), spare
        for i in candidates:
            extra = min(reach - counts[i], max(1, budget * portions[i] // mass), spare)
            counts[i] = counts[i] + extra
            spare = spare - extra
    return np.array([reach] + counts)


def ragged(own_key, amount, total, bound, lean):
    if amount == 2:
        one = jax.random.randint(own_key, (), max(1, total - bound), min(bound, total - 1) + 1)
        return jnp.stack([one, total - one])
    sizes = jnp.asarray(length_profile(amount, total, bound, lean), jnp.int32)
    twos = (amount - 1) // 2
    giver, sink = sizes[1:1 + 2 * twos:2], sizes[2:2 + 2 * twos:2]
    slack = jnp.minimum(giver - 1, bound - sink)
    shifted = jax.random.randint(jax.random.fold_in(own_key, 1), (twos,), 0, 1 << 20) % (slack + 1)
    sizes = sizes.at[1:1 + 2 * twos:2].set(giver - shifted).at[2:2 + 2 * twos:2].set(sink + shifted)
    return sizes[jax.random.permutation(jax.random.fold_in(own_key, 2), amount)]


def shared_out(key, own, number, rows, number_of, top, most, lean):
    ranking = jax.random.permutation(key, number_of)
    packed, common = shares(number_of, rows * top, most, lean, True), shares(number_of, rows * top, most, lean, False)
    places = jnp.arange(number_of)

    def named(tallies, offset_by):
        used = int((tallies > 0).sum())
        fixed = max(1, used // 4)
        shifted = fixed + (places - fixed + offset_by * (used - fixed)) % max(1, number_of - fixed)
        return jnp.zeros((number_of,), jnp.int32).at[ranking[jnp.where(places < fixed, places, shifted)]].set(jnp.asarray(tallies, jnp.int32))

    tallies = jnp.where(number % 4 == 0, named(packed, number // 4), named(common, number - number // 4 - 1))
    mixed = jax.random.permutation(jax.random.fold_in(own, 3), number_of)
    donor, taker = mixed[0:number_of // 2 * 2:2], mixed[1:number_of // 2 * 2:2]
    margin = jnp.minimum(tallies[donor] - 1, most - tallies[taker]) // 2
    margin = jnp.where((donor == ranking[0]) | (taker == ranking[0]) | (tallies[taker] == 0), 0, jnp.maximum(margin, 0))
    shifted = jax.random.randint(jax.random.fold_in(own, 4), (number_of // 2,), 0, 1 << 20) % (margin + 1)
    tallies = tallies.at[donor].add(-shifted).at[taker].add(shifted)
    labels = jnp.searchsorted(jnp.cumsum(tallies), jnp.arange(rows * top), side="right").astype(jnp.int32)
    listing = labels.reshape(top, rows).T
    listing = listing[jax.random.permutation(jax.random.fold_in(own, 1), rows)]
    offset_by = jax.random.randint(jax.random.fold_in(own, 2), (rows, 1), 0, top)
    return jnp.take_along_axis(listing, (jnp.arange(top)[None, :] + offset_by) % top, axis=1)


def shares(number_of, total, bound, lean, full):
    portions = [(1 << 20) // math.isqrt(standing ** lean) + 1 for standing in range(1, number_of + 1)]
    largest = bound if full else min(bound, max(-(-total // number_of), total * portions[0] // sum(portions)))
    least = 1 if total - largest >= number_of - 1 else 0
    holding, surplus = [largest] + [least] * (number_of - 1), total - largest - least * (number_of - 1)
    while surplus > 0:
        candidates = [i for i in range(1, number_of) if holding[i] < largest] or [i for i in range(1, number_of) if holding[i] < bound]
        whole, budget = sum([portions[i] for i in candidates]), surplus
        for i in candidates:
            addition = min(bound - holding[i], max(1, budget * portions[i] // whole), surplus)
            holding[i] = holding[i] + addition
            surplus = surplus - addition
    return np.array(holding)


def centred(stream_key, extent, scale, reach, cuts=(), dtype=jnp.bfloat16):
    entries = jax.random.normal(stream_key, extent, jnp.float32) * scale
    if len(cuts) > 0:
        entries = shard_levels(stream_key, extent, cuts, -0.22, 0.18) * entries
    return jnp.clip(entries, min=-reach, max=reach).astype(dtype)


def setup_inputs(seed: int = 0) -> dict:
    keys = jax.random.split(jax.random.key(seed), 15)
    q_new = draw_q_new(jax.random.fold_in(keys[14], 71), 0)
    k_cache = draw_k_cache(jax.random.fold_in(keys[14], 71), 0)
    value_cache = centred(keys[2], (STREAM_COUNT, KEY_VALUE_HEADS, CACHE_POSITIONS, HEAD_SIZE), 2.0, 12.0, ((0, 128), (1, 4)))
    k_new = draw_k_new(jax.random.fold_in(keys[14], 71), 0)
    new_value_rows = centred(keys[4], (STREAM_COUNT, NEW_TOKEN_ROWS, KEY_VALUE_HEADS * HEAD_SIZE), 2.0, 12.0, ((0, 128), (2, 4)))
    cache_len = ragged(keys[5], STREAM_COUNT, STREAM_COUNT * CACHE_POSITIONS // 2, CACHE_POSITIONS, 2).astype(jnp.int32)
    hidden_in = draw_hidden_in(jax.random.fold_in(keys[14], 71), 0)
    out_proj = centred(keys[7], (QUERY_HEADS * HEAD_SIZE, D), (QUERY_HEADS * HEAD_SIZE) ** -0.5, 0.09375, ((0, 4), (1, 2)))
    norm_gain = jnp.clip(1.0 + 0.18 * jax.random.normal(keys[8], (D,), jnp.float32), 0.1, 1.9)
    expert_ids_keys = jax.random.split(jax.random.fold_in(keys[9], 1), STREAM_COUNT * NEW_TOKEN_ROWS // ROWB)
    expert_ids_turns = jax.random.permutation(jax.random.fold_in(keys[9], 3), STREAM_COUNT * NEW_TOKEN_ROWS // ROWB)
    expert_ids = jax.vmap(lambda own, number: shared_out(jax.random.fold_in(keys[9], 2), own, number, ROWB, EXPERTS, TOPK, MOST, 2))(expert_ids_keys, expert_ids_turns).reshape((STREAM_COUNT, NEW_TOKEN_ROWS, TOPK))
    gate_wts = jnp.clip(jnp.exp(math.log(1.0) - 2.9957323 * jax.random.uniform(keys[10], (STREAM_COUNT, NEW_TOKEN_ROWS, TOPK), jnp.float32) ** shard_levels(keys[10], (STREAM_COUNT, NEW_TOKEN_ROWS, TOPK), ((0, 128), (1, 4)), -0.2, 0.2)), 0.05, 1.0)
    w_gate = centred(keys[11], (EXPERTS, D, FF), D ** -0.5, 0.125, ((0, 128), (2, 4)))
    w_up = centred(keys[12], (EXPERTS, D, FF), D ** -0.5, 0.125, ((0, 128), (2, 4)))
    w_down = centred(keys[13], (EXPERTS, FF, D), FF ** -0.5, 0.21875, ((0, 128), (1, 4)))
    return {"q_new": q_new, "k_cache": k_cache, "value_cache": value_cache, "k_new": k_new, "new_value_rows": new_value_rows, "cache_len": cache_len, "hidden_in": hidden_in, "out_proj": out_proj, "norm_gain": norm_gain, "expert_ids": expert_ids, "gate_wts": gate_wts, "w_gate": w_gate, "w_up": w_up, "w_down": w_down}


def attend_stream(operands):
    query_rows, cached_key_rows, cached_value_rows, fresh_key_rows, fresh_value_rows, valid_len = operands
    query_groups = QUERY_HEADS // KEY_VALUE_HEADS
    joined_keys = jnp.concatenate([cached_key_rows, fresh_key_rows.reshape(NEW_TOKEN_ROWS, KEY_VALUE_HEADS, HEAD_SIZE).transpose(1, 0, 2)], axis=1)
    joined_values = jnp.concatenate([cached_value_rows, fresh_value_rows.reshape(NEW_TOKEN_ROWS, KEY_VALUE_HEADS, HEAD_SIZE).transpose(1, 0, 2)], axis=1)
    reshaped_rows = query_rows.reshape(NEW_TOKEN_ROWS, KEY_VALUE_HEADS, query_groups, HEAD_SIZE)
    scores = jnp.einsum('rjgd,jkd->jgrk', reshaped_rows.astype(jnp.float32), joined_keys.astype(jnp.float32)) / math.sqrt(HEAD_SIZE)
    key_pos = jnp.arange(CACHE_POSITIONS + NEW_TOKEN_ROWS)[None, :]
    row_pos = jnp.arange(NEW_TOKEN_ROWS)[:, None]
    visible = jnp.where(key_pos < CACHE_POSITIONS, key_pos < valid_len, key_pos - CACHE_POSITIONS <= row_pos)
    scores = jnp.where(visible, scores, -jnp.inf)
    highest = lax.optimization_barrier(jnp.max(scores, axis=-1, keepdims=True))
    exp_scores = jnp.exp(scores - highest)
    attn_probs = (exp_scores / lax.optimization_barrier(jnp.sum(exp_scores, axis=-1, keepdims=True))).astype(jnp.bfloat16)
    context = jnp.einsum('jgrk,jkd->rjgd', attn_probs.astype(jnp.float32), joined_values.astype(jnp.float32)).astype(jnp.bfloat16)
    return context.reshape(NEW_TOKEN_ROWS, QUERY_HEADS * HEAD_SIZE)

def reference(q_new, k_cache, value_cache, k_new, new_value_rows, cache_len, hidden_in, out_proj, norm_gain, expert_ids, gate_wts, w_gate, w_up, w_down):
    context = lax.map(attend_stream, (q_new, k_cache, value_cache, k_new, new_value_rows, cache_len))
    total_rows = STREAM_COUNT * NEW_TOKEN_ROWS
    attn_out = jnp.dot(context.reshape(total_rows, QUERY_HEADS * HEAD_SIZE), out_proj, preferred_element_type=jnp.float32)
    resid = hidden_in.reshape(total_rows, D).astype(jnp.float32) + attn_out
    normed = (resid * lax.rsqrt(lax.optimization_barrier(jnp.mean(resid * resid, axis=-1, keepdims=True)) + 1e-06) * norm_gain).astype(jnp.bfloat16)
    raw_wts = gate_wts.reshape(total_rows, TOPK)
    mixing = (raw_wts / lax.optimization_barrier(jnp.sum(raw_wts, axis=-1, keepdims=True))).astype(jnp.bfloat16)
    chosen = expert_ids.reshape(total_rows, TOPK).astype(jnp.int32)
    blocks = total_rows // ROWB
    by_block = chosen.reshape(blocks, ROWB * TOPK)
    one_hot = (by_block[:, :, None] == jnp.arange(EXPERTS).astype(jnp.int32)[None, None, :]).astype(jnp.int32)
    earlier = jnp.cumsum(one_hot, axis=1) - one_hot
    slot_index = lax.optimization_barrier(jnp.sum(earlier * one_hot, axis=-1))
    column = (jnp.arange(blocks).astype(jnp.int32)[:, None] * MOST + slot_index).reshape(-1).astype(jnp.int32)
    row_index = jnp.repeat(jnp.arange(total_rows).astype(jnp.int32), TOPK)
    expert_flat = chosen.reshape(-1)
    table = jnp.full((EXPERTS, blocks * MOST), total_rows, jnp.int32).at[expert_flat, column].set(row_index)
    wtable = jnp.zeros((EXPERTS, blocks * MOST), jnp.float32).at[expert_flat, column].set(mixing.reshape(-1).astype(jnp.float32))
    padded = jnp.concatenate([normed, jnp.zeros((1, D), jnp.bfloat16)], axis=0)

    def expert_step(running, operands):
        slot_rows, slot_wts, gate_mat, up_mat, down_mat = operands
        gathered = padded[slot_rows]
        gate_proj = jnp.dot(gathered, gate_mat, preferred_element_type=jnp.float32)
        up_proj = jnp.dot(gathered, up_mat, preferred_element_type=jnp.float32)
        hidden = (jax.nn.silu(gate_proj) * up_proj).astype(jnp.bfloat16)
        partial_value = jnp.einsum('nqf,qfd->nqd', hidden.reshape(-1, N_HEAD, FF_PART).astype(jnp.float32), down_mat.reshape(N_HEAD, FF_PART, D).astype(jnp.float32)).astype(jnp.bfloat16)
        addend = slot_wts[:, None] * lax.optimization_barrier(jnp.sum(partial_value.astype(jnp.float32), axis=1))
        return (running.at[slot_rows].add(addend), None)
    running = jnp.zeros((total_rows + 1, D), jnp.float32)
    running = lax.scan(expert_step, running, (table, wtable, w_gate, w_up, w_down))[0]
    layer_out = (resid + running[:total_rows]).astype(jnp.bfloat16)
    return layer_out.reshape(STREAM_COUNT, NEW_TOKEN_ROWS, D)
```

```python
import math

import jax
import jax.numpy as jnp
from jax import lax
from jax.sharding import Mesh
from jax.sharding import PartitionSpec as P

STREAM = ("side", "x", "yp", "yq", "zl")
NEAR = ("yp", "head")
FAR = ("side", "x", "yq", "zl")


def attend(q_new, k_cache, value_cache, k_new, new_value_rows, cache_len):
    q_rows = q_new.shape[1]
    head_dim = k_cache.shape[3]
    cached_part = k_cache.shape[2]
    query_groups = q_new.shape[2] // head_dim
    joined_keys = jnp.concatenate([k_cache[0, 0], k_new[0]], axis=0)
    joined_values = jnp.concatenate([value_cache[0, 0], new_value_rows[0]], axis=0)
    query_rows = q_new[0].reshape(q_rows, query_groups, head_dim)
    scores = jnp.einsum(
        "rgd,kd->grk", query_rows, joined_keys, preferred_element_type=jnp.float32
    ) / math.sqrt(head_dim)
    key_pos = jnp.arange(cached_part + q_rows)[None, :]
    row_pos = jnp.arange(q_rows)[:, None]
    visible = jnp.where(
        key_pos < cached_part, key_pos < cache_len[0], key_pos - cached_part <= row_pos
    )
    scores = jnp.where(visible[None], scores, -jnp.inf)
    highest = jnp.max(scores, axis=-1, keepdims=True)
    exp_scores = jnp.exp(scores - highest)
    attn_probs = (exp_scores / jnp.sum(exp_scores, axis=-1, keepdims=True)).astype(jnp.bfloat16)
    context = jnp.einsum(
        "grk,kd->rgd", attn_probs, joined_values, preferred_element_type=jnp.float32
    ).astype(jnp.bfloat16)
    return context.reshape(q_rows, query_groups * head_dim)


def a2a(value, axes):
    return lax.all_to_all(value, axes, split_axis=0, concat_axis=0, tiled=True)


def slot_codes(chosen):
    same = chosen[:, :, None, None] == chosen[None, None, :, :]
    rows = jnp.arange(chosen.shape[0])
    before = (rows[None, :] < rows[:, None])[:, None, :, None]
    rank = jnp.sum((same & before).astype(jnp.int32), axis=(2, 3))
    return chosen * 2 + rank


def shards(
    q_new,
    k_cache,
    value_cache,
    k_new,
    new_value_rows,
    cache_len,
    hidden_in,
    out_proj,
    norm_gain,
    expert_ids,
    gate_wts,
    w_gate,
    w_up,
    w_down,
):
    width = hidden_in.shape[2]
    block = hidden_in.shape[1]
    side = lax.axis_index("side")
    quarters = lax.axis_size("head")
    near = lax.axis_size(NEAR)
    far = lax.axis_size(FAR)
    slots = 2 * near

    partner_proj = lax.ppermute(out_proj, "side", [(0, 1), (1, 0)])
    context = attend(q_new, k_cache, value_cache, k_new, new_value_rows, cache_len)
    own = jnp.dot(context, out_proj, preferred_element_type=jnp.float32)
    partner = jnp.dot(context, partner_proj, preferred_element_type=jnp.float32)
    full_rows = jnp.concatenate(
        [jnp.where(side == 0, own, partner), jnp.where(side == 0, partner, own)], axis=1
    ).astype(jnp.bfloat16)
    pieces = a2a(full_rows.reshape(quarters, block, width), "head")
    resid = hidden_in[0].astype(jnp.float32) + jnp.sum(pieces.astype(jnp.float32), axis=0)
    normed = (
        resid * lax.rsqrt(jnp.mean(resid * resid, axis=-1, keepdims=True) + 1e-06) * norm_gain
    ).astype(jnp.bfloat16)

    raw_wts = gate_wts[0]
    mixing = (raw_wts / jnp.sum(raw_wts, axis=-1, keepdims=True)).astype(jnp.bfloat16)
    top_k = mixing.shape[1]
    codes = slot_codes(expert_ids[0]).astype(jnp.bfloat16)
    extra = jnp.pad(jnp.concatenate([codes, mixing], axis=1), ((0, 0), (0, 128 - 2 * top_k)))
    payload = jnp.concatenate([normed, extra], axis=1)
    gathered = a2a(jnp.broadcast_to(payload[None], (near,) + payload.shape), NEAR)
    gathered = gathered.reshape(near * block, width + 128)
    rows = gathered[:, :width]
    code = gathered[:, width : width + top_k].astype(jnp.int32)
    mix = gathered[:, width + top_k : width + 2 * top_k]

    place = jnp.arange(far)
    per_side = far // 2
    per_x = per_side // lax.axis_size("x")
    pair = per_x // lax.axis_size("yq")
    ys = lax.axis_size("yp") * lax.axis_size("yq")
    xs = lax.axis_size("x")
    expert = (
        ((place // per_side) * xs + (place // per_x) % xs) * ys
        + lax.axis_index("yp") * lax.axis_size("yq")
        + (place // pair) % lax.axis_size("yq")
    ) * pair + place % pair
    wanted = (expert[:, None] * 2 + jnp.arange(2)[None, :]).reshape(-1)
    hit = wanted[:, None, None] == code.T[None, :, :]
    takes = jnp.any(hit, axis=1)
    weight = jnp.sum(jnp.where(hit, mix.T[None].astype(jnp.float32), 0.0), axis=1)
    own_block = (jnp.arange(near)[:, None] == (jnp.arange(near * block) // block)[None, :])
    dispatch = (takes[:, None, :] & own_block[None]).astype(jnp.bfloat16)
    combine = jnp.where(own_block[None], weight[:, None, :], 0.0).astype(jnp.bfloat16)
    dispatch = dispatch.reshape(far * slots, near * block)
    combine = combine.reshape(far * slots, near * block)

    outgoing = jnp.dot(dispatch, rows, preferred_element_type=jnp.float32).astype(jnp.bfloat16)
    flat_rows = a2a(outgoing.reshape(far, slots, width), FAR).reshape(far * slots, width)
    gate_proj = jnp.dot(flat_rows, w_gate[0], preferred_element_type=jnp.float32)
    up_proj = jnp.dot(flat_rows, w_up[0], preferred_element_type=jnp.float32)
    hidden = (jax.nn.silu(gate_proj) * up_proj).astype(jnp.bfloat16)
    partial_value = jnp.dot(hidden, w_down[0], preferred_element_type=jnp.float32).astype(
        jnp.bfloat16
    )
    returned = a2a(partial_value.reshape(far, slots, width), FAR).reshape(far * slots, width)
    weighted = lax.dot_general(
        combine, returned, (((0,), (0,)), ((), ())), preferred_element_type=jnp.float32
    ).astype(jnp.bfloat16)
    parts = a2a(weighted.reshape(near, block, width), NEAR)
    moe_out = jnp.sum(parts.astype(jnp.float32), axis=0)
    return (resid + moe_out).astype(jnp.bfloat16)[None]


def solution(mesh):
    fine = Mesh(
        mesh.devices.reshape(2, 4, 4, 2, 2, 4), ("side", "x", "yp", "yq", "zl", "head")
    )
    in_specs = (
        P(STREAM, None, "head"),
        P(STREAM, "head", None, None),
        P(STREAM, "head", None, None),
        P(STREAM, None, "head"),
        P(STREAM, None, "head"),
        P(STREAM),
        P(STREAM, "head", None),
        P("head", "side"),
        P(),
        P(STREAM, "head", None),
        P(STREAM, "head", None),
        P(STREAM, None, "head"),
        P(STREAM, None, "head"),
        P(STREAM, "head", None),
    )
    out_specs = P(STREAM, "head", None)
    return jax.shard_map(shards, mesh=fine, in_specs=in_specs, out_specs=out_specs, check_vma=False)
```

```python
import math

import jax
import jax.numpy as jnp
from jax import lax
from jax.experimental import pallas as pl
from jax.experimental.pallas import tpu as pltpu
from jax.sharding import Mesh
from jax.sharding import PartitionSpec as P

STREAM = ("side", "x", "yp", "yq", "zl")
NEAR = ("head", "yp")
FAR = ("x", "yq", "zl", "side")


def attention_kernel(
    len_ref,
    q_hbm,
    k_hbm,
    v_hbm,
    kn_hbm,
    vn_hbm,
    proj_hbm,
    ctx_ref,
    own_ref,
    q_ref,
    k_ref,
    v_ref,
    kn_ref,
    vn_ref,
    proj_ref,
    sems,
):
    pairs = (
        (q_hbm, q_ref),
        (k_hbm, k_ref),
        (kn_hbm, kn_ref),
        (v_hbm, v_ref),
        (vn_hbm, vn_ref),
        (proj_hbm, proj_ref),
    )
    loads = [
        pltpu.make_async_copy(source, target, sems.at[index])
        for index, (source, target) in enumerate(pairs)
    ]
    for load in loads:
        load.start()
    for load in loads[:-1]:
        load.wait()
    rows = q_ref.shape[1]
    cached, size = k_ref.shape[2], k_ref.shape[3]
    groups = q_ref.shape[2] // size
    per = 2
    scale = 1.0 / math.sqrt(size)
    old_key, new_key = k_ref[0, 0], kn_ref[0]
    old_val, new_val = v_ref[0, 0], vn_ref[0]
    contract = (((1,), (1,)), ((), ()))
    key_pos = lax.broadcasted_iota(jnp.int32, (per * rows, cached), 1)
    old_seen = key_pos < len_ref[0]
    row_pos = lax.broadcasted_iota(jnp.int32, (per * rows, rows), 0) % rows
    new_seen = lax.broadcasted_iota(jnp.int32, (per * rows, rows), 1) <= row_pos
    for start in range(0, groups, per):
        query = jnp.concatenate(
            [q_ref[0, :, (start + g) * size : (start + g + 1) * size] for g in range(per)], axis=0
        )
        old = lax.dot_general(query, old_key, contract, preferred_element_type=jnp.float32) * scale
        new = lax.dot_general(query, new_key, contract, preferred_element_type=jnp.float32) * scale
        old = jnp.where(old_seen, old, -jnp.inf)
        new = jnp.where(new_seen, new, -jnp.inf)
        highest = jnp.maximum(
            jnp.max(old, axis=1, keepdims=True), jnp.max(new, axis=1, keepdims=True)
        )
        old = jnp.exp(old - highest)
        new = jnp.exp(new - highest)
        total = jnp.sum(old, axis=1, keepdims=True) + jnp.sum(new, axis=1, keepdims=True)
        share = 1.0 / total
        context = jnp.dot(
            (old * share).astype(jnp.bfloat16), old_val, preferred_element_type=jnp.float32
        ) + jnp.dot((new * share).astype(jnp.bfloat16), new_val, preferred_element_type=jnp.float32)
        context = context.astype(jnp.bfloat16)
        for g in range(per):
            ctx_ref[:, (start + g) * size : (start + g + 1) * size] = context[
                g * rows : (g + 1) * rows
            ]
    loads[-1].wait()
    own_ref[...] = jnp.dot(
        ctx_ref[...], proj_ref[...], preferred_element_type=jnp.float32
    ).astype(jnp.bfloat16)


def project_kernel(side_ref, ctx_ref, proj_any, own_ref, out_ref, proj_ref, sem):
    load = pltpu.make_async_copy(proj_any, proj_ref, sem)
    load.start()
    load.wait()
    half = proj_ref.shape[1]
    block = out_ref.shape[1]
    side = side_ref[0]
    partner = jnp.dot(
        ctx_ref[...], proj_ref[...], preferred_element_type=jnp.float32
    ).astype(jnp.bfloat16)
    mine = pl.ds(pl.multiple_of(side * half, half), half)
    other = pl.ds(pl.multiple_of((1 - side) * half, half), half)
    for part in range(out_ref.shape[0]):
        take = slice(part * block, (part + 1) * block)
        out_ref[part, :, mine] = own_ref[take]
        out_ref[part, :, other] = partner[take]


def expert_kernel(rows_ref, gate_ref, up_ref, down_ref, out_ref):
    contract = (((1,), (1,)), ((), ()))
    rows = rows_ref[...]
    gate = lax.dot_general(rows, gate_ref[...], contract, preferred_element_type=jnp.float32)
    up = lax.dot_general(rows, up_ref[...], contract, preferred_element_type=jnp.float32)
    hidden = (gate / (1.0 + jnp.exp(-gate)) * up).astype(jnp.bfloat16)
    out_ref[...] = jnp.dot(hidden, down_ref[...], preferred_element_type=jnp.float32).astype(
        jnp.bfloat16
    )


def combine_kernel(combine_ref, rows_ref, out_ref):
    out_ref[...] = jnp.dot(
        combine_ref[...], rows_ref[...], preferred_element_type=jnp.float32
    ).astype(jnp.bfloat16)


def in_vmem():
    return pl.BlockSpec(memory_space=pltpu.VMEM)


def in_smem():
    return pl.BlockSpec(memory_space=pltpu.SMEM)


def a2a(value, axes):
    return lax.all_to_all(value, axes, split_axis=0, concat_axis=0, tiled=True)


def slot_codes(chosen):
    same = chosen[:, :, None, None] == chosen[None, None, :, :]
    rows = jnp.arange(chosen.shape[0])
    before = (rows[None, :] < rows[:, None])[:, None, :, None]
    rank = jnp.sum((same & before).astype(jnp.int32), axis=(2, 3))
    return chosen * 2 + rank


def shards(
    q_new,
    k_cache,
    value_cache,
    k_new,
    new_value_rows,
    cache_len,
    hidden_in,
    out_proj,
    norm_gain,
    expert_ids,
    gate_wts,
    w_gate,
    w_up,
    w_down,
):
    width = hidden_in.shape[2]
    block = hidden_in.shape[1]
    side = lax.axis_index("side")
    quarters = lax.axis_size("head")
    near = lax.axis_size(NEAR)
    far = lax.axis_size(FAR)
    slots = 2 * near

    partner_proj = lax.ppermute(out_proj, "side", [(0, 1), (1, 0)])
    half = out_proj.shape[1]
    rows_here = q_new.shape[1]
    context, own = pl.pallas_call(
        attention_kernel,
        in_specs=[in_smem()] + [pl.BlockSpec(memory_space=pltpu.HBM)] * 6,
        out_specs=[in_vmem()] * 2,
        scratch_shapes=[
            pltpu.VMEM(value.shape, jnp.bfloat16)
            for value in (q_new, k_cache, value_cache, k_new, new_value_rows, out_proj)
        ]
        + [pltpu.SemaphoreType.DMA((6,))],
        out_shape=[
            jax.ShapeDtypeStruct((rows_here, q_new.shape[2]), jnp.bfloat16),
            jax.ShapeDtypeStruct((rows_here, half), jnp.bfloat16),
        ],
        cost_estimate=pl.CostEstimate(
            flops=400_000_000, bytes_accessed=3_000_000, transcendentals=300_000
        ),
        compiler_params=pltpu.CompilerParams(vmem_limit_bytes=12 << 20),
        name="attention",
    )(
        cache_len,
        *(
            pltpu.with_memory_space_constraint(value, pltpu.HBM)
            for value in (q_new, k_cache, value_cache, k_new, new_value_rows, out_proj)
        ),
    )
    full_rows = pl.pallas_call(
        project_kernel,
        in_specs=[in_smem(), in_vmem(), pl.BlockSpec(memory_space=pl.ANY), in_vmem()],
        out_specs=in_vmem(),
        scratch_shapes=[pltpu.VMEM(out_proj.shape, jnp.bfloat16), pltpu.SemaphoreType.DMA],
        out_shape=jax.ShapeDtypeStruct((quarters, block, width), jnp.bfloat16),
        cost_estimate=pl.CostEstimate(
            flops=140_000_000, bytes_accessed=2_500_000, transcendentals=0
        ),
        compiler_params=pltpu.CompilerParams(vmem_limit_bytes=12 << 20),
        name="project",
    )(side.reshape(1), context, partner_proj, own)
    pieces = a2a(full_rows, "head")
    resid = hidden_in[0].astype(jnp.float32) + jnp.sum(pieces.astype(jnp.float32), axis=0)
    normed = (
        resid * lax.rsqrt(jnp.mean(resid * resid, axis=-1, keepdims=True) + 1e-06) * norm_gain
    ).astype(jnp.bfloat16)

    raw_wts = gate_wts[0]
    mixing = (raw_wts / jnp.sum(raw_wts, axis=-1, keepdims=True)).astype(jnp.bfloat16)
    top_k = mixing.shape[1]
    codes = slot_codes(expert_ids[0]).astype(jnp.bfloat16)
    extra = jnp.pad(jnp.concatenate([codes, mixing], axis=1), ((0, 0), (0, 128 - 2 * top_k)))
    payload = jnp.concatenate([normed, extra], axis=1)
    gathered = a2a(jnp.broadcast_to(payload[None], (near,) + payload.shape), NEAR)
    gathered = gathered.reshape(near * block, width + 128)
    rows = gathered[:, :width]
    code = gathered[:, width : width + top_k].astype(jnp.int32)
    mix = gathered[:, width + top_k : width + 2 * top_k]

    place = jnp.arange(far)
    xs, ps, qs, zs = (lax.axis_size(name) for name in ("x", "yp", "yq", "zl"))
    sides = lax.axis_size("side")
    at_z = (place // sides) % zs
    at_q = (place // (sides * zs)) % qs
    at_x = place // (sides * zs * qs)
    expert = (
        ((place % sides) * xs + at_x) * (ps * qs) + lax.axis_index("yp") * qs + at_q
    ) * zs + at_z
    wanted = (expert[:, None] * 2 + jnp.arange(2)[None, :]).reshape(-1)
    hit = wanted[:, None, None] == code.T[None, :, :]
    takes = jnp.any(hit, axis=1)
    weight = jnp.sum(jnp.where(hit, mix.T[None].astype(jnp.float32), 0.0), axis=1)
    own_block = (jnp.arange(near)[:, None] == (jnp.arange(near * block) // block)[None, :])
    dispatch = (takes[:, None, :] & own_block[None]).astype(jnp.bfloat16)
    combine = jnp.where(own_block.T[:, None, :], weight.T[:, :, None], 0.0).astype(jnp.bfloat16)
    dispatch = dispatch.reshape(far * slots, near * block)
    combine = combine.reshape(near * block, far * slots)

    outgoing = jnp.dot(dispatch, rows, preferred_element_type=jnp.float32).astype(jnp.bfloat16)
    flat_rows = a2a(outgoing.reshape(far, slots, width), FAR).reshape(far * slots, width)
    tile = 256
    part = w_gate.shape[2]
    partial_value = pl.pallas_call(
        expert_kernel,
        grid=(far * slots // tile,),
        in_specs=[
            pl.BlockSpec((tile, width), lambda i: (i, 0)),
            pl.BlockSpec((part, width), lambda i: (0, 0)),
            pl.BlockSpec((part, width), lambda i: (0, 0)),
            pl.BlockSpec((part, width), lambda i: (0, 0)),
        ],
        out_specs=pl.BlockSpec((tile, width), lambda i: (i, 0)),
        out_shape=pltpu.HBM((far * slots, width), jnp.bfloat16),
        cost_estimate=pl.CostEstimate(
            flops=2_500_000_000, bytes_accessed=11_000_000, transcendentals=200_000
        ),
        compiler_params=pltpu.CompilerParams(vmem_limit_bytes=24 << 20),
        name="experts",
    )(flat_rows, w_gate[0].T, w_up[0].T, w_down[0])
    returned = a2a(partial_value.reshape(far, slots, width), FAR).reshape(far * slots, width)
    columns = 512
    weighted = pl.pallas_call(
        combine_kernel,
        grid=(width // columns,),
        in_specs=[
            pl.BlockSpec((near * block, far * slots), lambda i: (0, 0)),
            pl.BlockSpec((far * slots, columns), lambda i: (0, i)),
        ],
        out_specs=pl.BlockSpec((near * block, columns), lambda i: (0, i)),
        out_shape=jax.ShapeDtypeStruct((near * block, width), jnp.bfloat16),
        cost_estimate=pl.CostEstimate(
            flops=1_100_000_000, bytes_accessed=6_000_000, transcendentals=0
        ),
        compiler_params=pltpu.CompilerParams(vmem_limit_bytes=16 << 20),
        name="combine",
    )(combine, returned)
    parts = a2a(weighted.reshape(near, block, width), NEAR)
    moe_out = jnp.sum(parts.astype(jnp.float32), axis=0)
    return (resid + moe_out).astype(jnp.bfloat16)[None]


def solution(mesh):
    fine = Mesh(
        mesh.devices.reshape(2, 4, 4, 2, 2, 4), ("side", "x", "yp", "yq", "zl", "head")
    )
    in_specs = (
        P(STREAM, None, "head"),
        P(STREAM, "head", None, None),
        P(STREAM, "head", None, None),
        P(STREAM, None, "head"),
        P(STREAM, None, "head"),
        P(STREAM),
        P(STREAM, "head", None),
        P("head", "side"),
        P(),
        P(STREAM, "head", None),
        P(STREAM, "head", None),
        P(STREAM, None, "head"),
        P(STREAM, None, "head"),
        P(STREAM, "head", None),
    )
    out_specs = P(STREAM, "head", None)
    return jax.shard_map(shards, mesh=fine, in_specs=in_specs, out_specs=out_specs, check_vma=False)
```

```python
import math

import jax
import jax.numpy as jnp
from jax import lax
from jax.experimental import pallas as pl
from jax.experimental.pallas import tpu as pltpu
from jax.sharding import Mesh
from jax.sharding import PartitionSpec as P

STREAM = ("side", "x", "yp", "yq", "zl")
NEAR = ("head", "yp")
FAR = ("x", "yq", "zl", "side")


def attention_kernel(
    len_ref,
    q_hbm,
    k_hbm,
    v_hbm,
    kn_hbm,
    vn_hbm,
    proj_hbm,
    ctx_ref,
    own_ref,
    q_ref,
    k_ref,
    v_ref,
    kn_ref,
    vn_ref,
    proj_ref,
    sems,
):
    pairs = (
        (q_hbm, q_ref),
        (k_hbm, k_ref),
        (kn_hbm, kn_ref),
        (v_hbm, v_ref),
        (vn_hbm, vn_ref),
        (proj_hbm, proj_ref),
    )
    loads = [
        pltpu.make_async_copy(source, target, sems.at[index])
        for index, (source, target) in enumerate(pairs)
    ]
    for load in loads:
        load.start()
    for load in loads[:-1]:
        load.wait()
    rows = q_ref.shape[1]
    cached, size = k_ref.shape[2], k_ref.shape[3]
    groups = q_ref.shape[2] // size
    per = 2
    scale = 1.0 / math.sqrt(size)
    old_key, new_key = k_ref[0, 0], kn_ref[0]
    old_val, new_val = v_ref[0, 0], vn_ref[0]
    contract = (((1,), (1,)), ((), ()))
    key_pos = lax.broadcasted_iota(jnp.int32, (per * rows, cached), 1)
    old_seen = key_pos < len_ref[0]
    row_pos = lax.broadcasted_iota(jnp.int32, (per * rows, rows), 0) % rows
    new_seen = lax.broadcasted_iota(jnp.int32, (per * rows, rows), 1) <= row_pos
    for start in range(0, groups, per):
        query = jnp.concatenate(
            [q_ref[0, :, (start + g) * size : (start + g + 1) * size] for g in range(per)], axis=0
        )
        old = lax.dot_general(query, old_key, contract, preferred_element_type=jnp.float32) * scale
        new = lax.dot_general(query, new_key, contract, preferred_element_type=jnp.float32) * scale
        old = jnp.where(old_seen, old, -jnp.inf)
        new = jnp.where(new_seen, new, -jnp.inf)
        highest = jnp.maximum(
            jnp.max(old, axis=1, keepdims=True), jnp.max(new, axis=1, keepdims=True)
        )
        old = jnp.exp(old - highest)
        new = jnp.exp(new - highest)
        total = jnp.sum(old, axis=1, keepdims=True) + jnp.sum(new, axis=1, keepdims=True)
        share = 1.0 / total
        context = jnp.dot(
            (old * share).astype(jnp.bfloat16), old_val, preferred_element_type=jnp.float32
        ) + jnp.dot((new * share).astype(jnp.bfloat16), new_val, preferred_element_type=jnp.float32)
        context = context.astype(jnp.bfloat16)
        for g in range(per):
            ctx_ref[:, (start + g) * size : (start + g + 1) * size] = context[
                g * rows : (g + 1) * rows
            ]
    loads[-1].wait()
    own_ref[...] = jnp.dot(
        ctx_ref[...], proj_ref[...], preferred_element_type=jnp.float32
    ).astype(jnp.bfloat16)


def project_kernel(side_ref, ctx_ref, proj_any, own_ref, out_ref, proj_ref, sem):
    load = pltpu.make_async_copy(proj_any, proj_ref, sem)
    load.start()
    load.wait()
    half = proj_ref.shape[1]
    block = out_ref.shape[1]
    side = side_ref[0]
    partner = jnp.dot(
        ctx_ref[...], proj_ref[...], preferred_element_type=jnp.float32
    ).astype(jnp.bfloat16)
    mine = pl.ds(pl.multiple_of(side * half, half), half)
    other = pl.ds(pl.multiple_of((1 - side) * half, half), half)
    for part in range(out_ref.shape[0]):
        take = slice(part * block, (part + 1) * block)
        out_ref[part, :, mine] = own_ref[take]
        out_ref[part, :, other] = partner[take]


def expert_kernel(rows_ref, gate_ref, up_ref, down_ref, out_ref):
    contract = (((1,), (1,)), ((), ()))
    rows = rows_ref[...]
    gate = lax.dot_general(rows, gate_ref[...], contract, preferred_element_type=jnp.float32)
    up = lax.dot_general(rows, up_ref[...], contract, preferred_element_type=jnp.float32)
    hidden = (gate / (1.0 + jnp.exp(-gate)) * up).astype(jnp.bfloat16)
    out_ref[...] = jnp.dot(hidden, down_ref[...], preferred_element_type=jnp.float32).astype(
        jnp.bfloat16
    )


def combine_kernel(combine_ref, rows_ref, out_ref):
    out_ref[...] = jnp.dot(
        combine_ref[...], rows_ref[...], preferred_element_type=jnp.float32
    ).astype(jnp.bfloat16)


def in_vmem():
    return pl.BlockSpec(memory_space=pltpu.VMEM)


def in_smem():
    return pl.BlockSpec(memory_space=pltpu.SMEM)


def a2a(value, axes):
    return lax.all_to_all(value, axes, split_axis=0, concat_axis=0, tiled=True)


def table_kernel(part_ref, routing_ref, dispatch_ref, combine_ref):
    top_k = routing_ref.shape[2] // 16
    blocks, block = routing_ref.shape[0], routing_ref.shape[1]
    rows = blocks * block
    columns = jnp.transpose(routing_ref[...].reshape(rows, routing_ref.shape[2]))
    chosen = columns[:top_k]
    weights = columns[top_k : 2 * top_k]
    mixing = (weights / jnp.sum(weights, axis=0, keepdims=True)).astype(jnp.bfloat16)
    mixing = mixing.astype(jnp.float32)
    sides, xs, ps, qs, zs = 2, 4, 4, 2, 2
    local = sides * xs * qs * zs
    place = lax.broadcasted_iota(jnp.int32, (local, rows), 0)
    at_z = (place // sides) % zs
    at_q = (place // (sides * zs)) % qs
    at_x = place // (sides * zs * qs)
    expert = (((place % sides) * xs + at_x) * (ps * qs) + part_ref[0] * qs + at_q) * zs + at_z
    expert = expert.astype(jnp.float32)
    named = jnp.zeros((local, rows), jnp.float32)
    weight = jnp.zeros((local, rows), jnp.float32)
    for k in range(top_k):
        hit = chosen[k : k + 1] == expert
        named = jnp.where(hit, 1.0, named)
        weight = jnp.where(hit, mixing[k : k + 1], weight)
    first = lax.broadcasted_iota(jnp.int32, (rows, rows), 0)
    second = lax.broadcasted_iota(jnp.int32, (rows, rows), 1)
    earlier = (first < second) & (first // block == second // block)
    rank = jnp.dot(
        named.astype(jnp.bfloat16),
        jnp.where(earlier, 1.0, 0.0).astype(jnp.bfloat16),
        preferred_element_type=jnp.float32,
    )
    own = lax.broadcasted_iota(jnp.int32, (blocks, rows), 0) == (
        lax.broadcasted_iota(jnp.int32, (blocks, rows), 1) // block
    )
    group = 128 // (2 * blocks)
    for start in range(0, local, group):
        tiles = []
        for e in range(start, start + group):
            for s in range(2):
                takes = (named[e : e + 1] > 0.5) & (jnp.abs(rank[e : e + 1] - s) < 0.5)
                at = (2 * e + s) * blocks
                dispatch_ref[at : at + blocks] = jnp.where(
                    own, jnp.where(takes, 1.0, 0.0), 0.0
                ).astype(jnp.bfloat16)
                tiles.append(jnp.where(own, jnp.where(takes, weight[e : e + 1], 0.0), 0.0))
        at = 2 * start * blocks
        combine_ref[:, at : at + 128] = jnp.transpose(jnp.concatenate(tiles, axis=0)).astype(
            jnp.bfloat16
        )


def shards(
    q_new,
    k_cache,
    value_cache,
    k_new,
    new_value_rows,
    cache_len,
    hidden_in,
    out_proj,
    norm_gain,
    expert_ids,
    gate_wts,
    w_gate,
    w_up,
    w_down,
):
    width = hidden_in.shape[2]
    block = hidden_in.shape[1]
    side = lax.axis_index("side")
    quarters = lax.axis_size("head")
    near = lax.axis_size(NEAR)
    far = lax.axis_size(FAR)
    slots = 2 * near

    top_k = expert_ids.shape[2]
    routing = jnp.concatenate([expert_ids[0].astype(jnp.float32), gate_wts[0]], axis=1)
    routing = jnp.pad(routing, ((0, 0), (0, 128 - 2 * top_k)))
    routing = a2a(jnp.broadcast_to(routing[None], (near,) + routing.shape), NEAR)
    partner_proj = lax.ppermute(out_proj, "side", [(0, 1), (1, 0)])
    half = out_proj.shape[1]
    rows_here = q_new.shape[1]
    context, own = pl.pallas_call(
        attention_kernel,
        in_specs=[in_smem()] + [pl.BlockSpec(memory_space=pltpu.HBM)] * 6,
        out_specs=[in_vmem()] * 2,
        scratch_shapes=[
            pltpu.VMEM(value.shape, jnp.bfloat16)
            for value in (q_new, k_cache, value_cache, k_new, new_value_rows, out_proj)
        ]
        + [pltpu.SemaphoreType.DMA((6,))],
        out_shape=[
            jax.ShapeDtypeStruct((rows_here, q_new.shape[2]), jnp.bfloat16),
            jax.ShapeDtypeStruct((rows_here, half), jnp.bfloat16),
        ],
        cost_estimate=pl.CostEstimate(
            flops=400_000_000, bytes_accessed=3_000_000, transcendentals=300_000
        ),
        compiler_params=pltpu.CompilerParams(vmem_limit_bytes=12 << 20),
        name="attention",
    )(
        cache_len,
        *(
            pltpu.with_memory_space_constraint(value, pltpu.HBM)
            for value in (q_new, k_cache, value_cache, k_new, new_value_rows, out_proj)
        ),
    )
    partner_proj, routing = lax.optimization_barrier((partner_proj, routing))
    full_rows = pl.pallas_call(
        project_kernel,
        in_specs=[in_smem(), in_vmem(), pl.BlockSpec(memory_space=pl.ANY), in_vmem()],
        out_specs=in_vmem(),
        scratch_shapes=[pltpu.VMEM(out_proj.shape, jnp.bfloat16), pltpu.SemaphoreType.DMA],
        out_shape=jax.ShapeDtypeStruct((quarters, block, width), jnp.bfloat16),
        cost_estimate=pl.CostEstimate(
            flops=140_000_000, bytes_accessed=2_500_000, transcendentals=0
        ),
        compiler_params=pltpu.CompilerParams(vmem_limit_bytes=12 << 20),
        name="project",
    )(side.reshape(1), context, partner_proj, own)
    pieces = a2a(full_rows, "head")
    resid = hidden_in[0].astype(jnp.float32) + jnp.sum(pieces.astype(jnp.float32), axis=0)
    normed = (
        resid * lax.rsqrt(jnp.mean(resid * resid, axis=-1, keepdims=True) + 1e-06) * norm_gain
    ).astype(jnp.bfloat16)

    rows = a2a(jnp.broadcast_to(normed[None], (near,) + normed.shape), NEAR)
    rows = rows.reshape(near * block, width)
    dispatch, combine = pl.pallas_call(
        table_kernel,
        in_specs=[in_smem(), in_vmem()],
        out_specs=[in_vmem()] * 2,
        out_shape=[
            jax.ShapeDtypeStruct((far * slots, near * block), jnp.bfloat16),
            jax.ShapeDtypeStruct((near * block, far * slots), jnp.bfloat16),
        ],
        cost_estimate=pl.CostEstimate(
            flops=1_000_000_000, bytes_accessed=1_200_000, transcendentals=0
        ),
        compiler_params=pltpu.CompilerParams(vmem_limit_bytes=12 << 20),
        name="tables",
    )(lax.axis_index("yp").reshape(1), routing)

    outgoing = jnp.dot(dispatch, rows, preferred_element_type=jnp.float32).astype(jnp.bfloat16)
    flat_rows = a2a(outgoing.reshape(far, slots, width), FAR).reshape(far * slots, width)
    tile = 256
    part = w_gate.shape[2]
    partial_value = pl.pallas_call(
        expert_kernel,
        grid=(far * slots // tile,),
        in_specs=[
            pl.BlockSpec((tile, width), lambda i: (i, 0)),
            pl.BlockSpec((part, width), lambda i: (0, 0)),
            pl.BlockSpec((part, width), lambda i: (0, 0)),
            pl.BlockSpec((part, width), lambda i: (0, 0)),
        ],
        out_specs=pl.BlockSpec((tile, width), lambda i: (i, 0)),
        out_shape=pltpu.HBM((far * slots, width), jnp.bfloat16),
        cost_estimate=pl.CostEstimate(
            flops=2_500_000_000, bytes_accessed=11_000_000, transcendentals=200_000
        ),
        compiler_params=pltpu.CompilerParams(vmem_limit_bytes=24 << 20),
        name="experts",
    )(flat_rows, w_gate[0].T, w_up[0].T, w_down[0])
    returned = a2a(partial_value.reshape(far, slots, width), FAR).reshape(far * slots, width)
    columns = 512
    weighted = pl.pallas_call(
        combine_kernel,
        grid=(width // columns,),
        in_specs=[
            pl.BlockSpec((near * block, far * slots), lambda i: (0, 0)),
            pl.BlockSpec((far * slots, columns), lambda i: (0, i)),
        ],
        out_specs=pl.BlockSpec((near * block, columns), lambda i: (0, i)),
        out_shape=jax.ShapeDtypeStruct((near * block, width), jnp.bfloat16),
        cost_estimate=pl.CostEstimate(
            flops=1_100_000_000, bytes_accessed=6_000_000, transcendentals=0
        ),
        compiler_params=pltpu.CompilerParams(vmem_limit_bytes=16 << 20),
        name="combine",
    )(combine, returned)
    parts = a2a(weighted.reshape(near, block, width), NEAR)
    moe_out = jnp.sum(parts.astype(jnp.float32), axis=0)
    return (resid + moe_out).astype(jnp.bfloat16)[None]


def solution(mesh):
    fine = Mesh(
        mesh.devices.reshape(2, 4, 4, 2, 2, 4), ("side", "x", "yp", "yq", "zl", "head")
    )
    in_specs = (
        P(STREAM, None, "head"),
        P(STREAM, "head", None, None),
        P(STREAM, "head", None, None),
        P(STREAM, None, "head"),
        P(STREAM, None, "head"),
        P(STREAM),
        P(STREAM, "head", None),
        P("head", "side"),
        P(),
        P(STREAM, "head", None),
        P(STREAM, "head", None),
        P(STREAM, None, "head"),
        P(STREAM, None, "head"),
        P(STREAM, "head", None),
    )
    out_specs = P(STREAM, "head", None)
    return jax.shard_map(shards, mesh=fine, in_specs=in_specs, out_specs=out_specs, check_vma=False)
```

```python
import math

import jax
import jax.numpy as jnp
from jax import lax
from jax.experimental import pallas as pl
from jax.experimental.pallas import tpu as pltpu
from jax.sharding import Mesh
from jax.sharding import PartitionSpec as P

STREAM = ("side", "x", "yp", "yq", "zl")
NEAR = ("head", "yp")
BACK = ("yp", "head")
FAR = ("x", "yq", "zl", "side")


def attention_kernel(
    len_ref,
    q_hbm,
    k_hbm,
    v_hbm,
    kn_hbm,
    vn_hbm,
    proj_hbm,
    ctx_ref,
    own_ref,
    q_ref,
    k_ref,
    v_ref,
    kn_ref,
    vn_ref,
    proj_ref,
    sems,
):
    pairs = (
        (q_hbm, q_ref),
        (k_hbm, k_ref),
        (kn_hbm, kn_ref),
        (v_hbm, v_ref),
        (vn_hbm, vn_ref),
        (proj_hbm, proj_ref),
    )
    loads = [
        pltpu.make_async_copy(source, target, sems.at[index])
        for index, (source, target) in enumerate(pairs)
    ]
    for load in loads:
        load.start()
    for load in loads[:-1]:
        load.wait()
    rows = q_ref.shape[1]
    cached, size = k_ref.shape[2], k_ref.shape[3]
    groups = q_ref.shape[2] // size
    per = 2
    scale = 1.0 / math.sqrt(size)
    old_key, new_key = k_ref[0, 0], kn_ref[0]
    old_val, new_val = v_ref[0, 0], vn_ref[0]
    contract = (((1,), (1,)), ((), ()))
    key_pos = lax.broadcasted_iota(jnp.int32, (per * rows, cached), 1)
    old_seen = key_pos < len_ref[0]
    row_pos = lax.broadcasted_iota(jnp.int32, (per * rows, rows), 0) % rows
    new_seen = lax.broadcasted_iota(jnp.int32, (per * rows, rows), 1) <= row_pos
    for start in range(0, groups, per):
        query = jnp.concatenate(
            [q_ref[0, :, (start + g) * size : (start + g + 1) * size] for g in range(per)], axis=0
        )
        old = lax.dot_general(query, old_key, contract, preferred_element_type=jnp.float32) * scale
        new = lax.dot_general(query, new_key, contract, preferred_element_type=jnp.float32) * scale
        old = jnp.where(old_seen, old, -jnp.inf)
        new = jnp.where(new_seen, new, -jnp.inf)
        highest = jnp.maximum(
            jnp.max(old, axis=1, keepdims=True), jnp.max(new, axis=1, keepdims=True)
        )
        old = jnp.exp(old - highest)
        new = jnp.exp(new - highest)
        total = jnp.sum(old, axis=1, keepdims=True) + jnp.sum(new, axis=1, keepdims=True)
        share = 1.0 / total
        context = jnp.dot(
            (old * share).astype(jnp.bfloat16), old_val, preferred_element_type=jnp.float32
        ) + jnp.dot((new * share).astype(jnp.bfloat16), new_val, preferred_element_type=jnp.float32)
        context = context.astype(jnp.bfloat16)
        for g in range(per):
            ctx_ref[:, (start + g) * size : (start + g + 1) * size] = context[
                g * rows : (g + 1) * rows
            ]
    loads[-1].wait()
    own_ref[...] = jnp.dot(
        ctx_ref[...], proj_ref[...], preferred_element_type=jnp.float32
    ).astype(jnp.bfloat16)


def project_kernel(side_ref, ctx_ref, proj_any, own_ref, out_ref, proj_ref, sem):
    load = pltpu.make_async_copy(proj_any, proj_ref, sem)
    load.start()
    load.wait()
    half = proj_ref.shape[1]
    block = out_ref.shape[1]
    side = side_ref[0]
    partner = jnp.dot(
        ctx_ref[...], proj_ref[...], preferred_element_type=jnp.float32
    ).astype(jnp.bfloat16)
    mine = pl.ds(pl.multiple_of(side * half, half), half)
    other = pl.ds(pl.multiple_of((1 - side) * half, half), half)
    for part in range(out_ref.shape[0]):
        take = slice(part * block, (part + 1) * block)
        out_ref[part, :, mine] = own_ref[take]
        out_ref[part, :, other] = partner[take]


def expert_kernel(rows_ref, gate_ref, up_ref, down_ref, out_ref):
    contract = (((1,), (1,)), ((), ()))
    rows = rows_ref[...]
    gate = lax.dot_general(rows, gate_ref[...], contract, preferred_element_type=jnp.float32)
    up = lax.dot_general(rows, up_ref[...], contract, preferred_element_type=jnp.float32)
    hidden = (gate / (1.0 + jnp.exp(-gate)) * up).astype(jnp.bfloat16)
    out_ref[...] = jnp.dot(hidden, down_ref[...], preferred_element_type=jnp.float32).astype(
        jnp.bfloat16
    )


def combine_kernel(combine_ref, rows_ref, out_ref):
    out_ref[...] = jnp.dot(
        combine_ref[...], rows_ref[...], preferred_element_type=jnp.float32
    ).astype(jnp.bfloat16)


def in_vmem():
    return pl.BlockSpec(memory_space=pltpu.VMEM)


def in_smem():
    return pl.BlockSpec(memory_space=pltpu.SMEM)


def a2a(value, axes):
    return lax.all_to_all(value, axes, split_axis=0, concat_axis=0, tiled=True)


def table_kernel(place_ref, routing_ref, dispatch_ref, combine_ref, sorted_ref):
    blocks, block = routing_ref.shape[0], routing_ref.shape[1]
    top_k = 8
    rows = blocks * block
    heads = 4
    for step in range(blocks):
        from_head = place_ref[0] ^ (step % heads)
        from_part = place_ref[1] ^ (step // heads)
        at = pl.multiple_of((from_head * (blocks // heads) + from_part) * block, block)
        sorted_ref[pl.ds(at, block), :] = routing_ref[step]
    columns = jnp.transpose(sorted_ref[...])
    chosen = columns[:top_k]
    weights = columns[top_k : 2 * top_k]
    mixing = (weights / jnp.sum(weights, axis=0, keepdims=True)).astype(jnp.bfloat16)
    mixing = mixing.astype(jnp.float32)
    sides, xs, ps, qs, zs = 2, 4, 4, 2, 2
    local = sides * xs * qs * zs
    place = lax.broadcasted_iota(jnp.int32, (local, rows), 0)
    at_z = (place // sides) % zs
    at_q = (place // (sides * zs)) % qs
    at_x = place // (sides * zs * qs)
    expert = (((place % sides) * xs + at_x) * (ps * qs) + place_ref[1] * qs + at_q) * zs + at_z
    expert = expert.astype(jnp.float32)
    named = jnp.zeros((local, rows), jnp.float32)
    weight = jnp.zeros((local, rows), jnp.float32)
    for k in range(top_k):
        hit = chosen[k : k + 1] == expert
        named = jnp.where(hit, 1.0, named)
        weight = jnp.where(hit, mixing[k : k + 1], weight)
    first = lax.broadcasted_iota(jnp.int32, (rows, rows), 0)
    second = lax.broadcasted_iota(jnp.int32, (rows, rows), 1)
    earlier = (first < second) & (first // block == second // block)
    rank = jnp.dot(
        named.astype(jnp.bfloat16),
        jnp.where(earlier, 1.0, 0.0).astype(jnp.bfloat16),
        preferred_element_type=jnp.float32,
    )
    own = lax.broadcasted_iota(jnp.int32, (blocks, rows), 0) == (
        lax.broadcasted_iota(jnp.int32, (blocks, rows), 1) // block
    )
    group = 128 // (2 * blocks)
    for start in range(0, local, group):
        tiles = []
        for e in range(start, start + group):
            for s in range(2):
                takes = (named[e : e + 1] > 0.5) & (jnp.abs(rank[e : e + 1] - s) < 0.5)
                at = (2 * e + s) * blocks
                dispatch_ref[at : at + blocks] = jnp.where(
                    own, jnp.where(takes, 1.0, 0.0), 0.0
                ).astype(jnp.bfloat16)
                tiles.append(jnp.where(own, jnp.where(takes, weight[e : e + 1], 0.0), 0.0))
        at = 2 * start * blocks
        turned = jnp.transpose(jnp.concatenate(tiles, axis=0)).astype(jnp.bfloat16)
        for source in range(blocks):
            target = (source % (blocks // heads)) * heads + source // (blocks // heads)
            combine_ref[target * block : (target + 1) * block, at : at + 128] = turned[
                source * block : (source + 1) * block
            ]


def shards(
    q_new,
    k_cache,
    value_cache,
    k_new,
    new_value_rows,
    cache_len,
    hidden_in,
    out_proj,
    norm_gain,
    expert_ids,
    gate_wts,
    w_gate,
    w_up,
    w_down,
):
    width = hidden_in.shape[2]
    block = hidden_in.shape[1]
    side = lax.axis_index("side")
    quarters = lax.axis_size("head")
    near = lax.axis_size(NEAR)
    far = lax.axis_size(FAR)
    slots = 2 * near

    top_k = expert_ids.shape[2]
    routing = jnp.concatenate([expert_ids[0].astype(jnp.float32), gate_wts[0]], axis=1)
    routing = jnp.pad(routing, ((0, 0), (0, 128 - 2 * top_k)))
    partner_proj = lax.ppermute(out_proj, "side", [(0, 1), (1, 0)])
    half = out_proj.shape[1]
    rows_here = q_new.shape[1]
    context, own = pl.pallas_call(
        attention_kernel,
        in_specs=[in_smem()] + [pl.BlockSpec(memory_space=pltpu.HBM)] * 6,
        out_specs=[in_vmem()] * 2,
        scratch_shapes=[
            pltpu.VMEM(value.shape, jnp.bfloat16)
            for value in (q_new, k_cache, value_cache, k_new, new_value_rows, out_proj)
        ]
        + [pltpu.SemaphoreType.DMA((6,))],
        out_shape=[
            jax.ShapeDtypeStruct((rows_here, q_new.shape[2]), jnp.bfloat16),
            jax.ShapeDtypeStruct((rows_here, half), jnp.bfloat16),
        ],
        cost_estimate=pl.CostEstimate(
            flops=400_000_000, bytes_accessed=3_000_000, transcendentals=300_000
        ),
        compiler_params=pltpu.CompilerParams(vmem_limit_bytes=12 << 20),
        name="attention",
    )(
        cache_len,
        *(
            pltpu.with_memory_space_constraint(value, pltpu.HBM)
            for value in (q_new, k_cache, value_cache, k_new, new_value_rows, out_proj)
        ),
    )
    full_rows = pl.pallas_call(
        project_kernel,
        in_specs=[in_smem(), in_vmem(), pl.BlockSpec(memory_space=pl.ANY), in_vmem()],
        out_specs=in_vmem(),
        scratch_shapes=[pltpu.VMEM(out_proj.shape, jnp.bfloat16), pltpu.SemaphoreType.DMA],
        out_shape=jax.ShapeDtypeStruct((quarters, block, width), jnp.bfloat16),
        cost_estimate=pl.CostEstimate(
            flops=140_000_000, bytes_accessed=2_500_000, transcendentals=0
        ),
        compiler_params=pltpu.CompilerParams(vmem_limit_bytes=12 << 20),
        name="project",
    )(side.reshape(1), context, partner_proj, own)
    pieces = a2a(full_rows, "head")
    resid = hidden_in[0].astype(jnp.float32) + jnp.sum(pieces.astype(jnp.float32), axis=0)
    normed = (
        resid * lax.rsqrt(jnp.mean(resid * resid, axis=-1, keepdims=True) + 1e-06) * norm_gain
    ).astype(jnp.bfloat16)

    spread = jnp.broadcast_to(normed[None], (near,) + normed.shape)
    spread, routing = lax.optimization_barrier((spread, routing[None]))
    rows = a2a(spread, NEAR)
    rows = rows.reshape(near * block, width)
    for axis in ("head", "yp"):
        for bit in (1, 2):
            pairs = [(i, i ^ bit) for i in range(lax.axis_size(axis))]
            routing = jnp.concatenate([routing, lax.ppermute(routing, axis, pairs)], axis=0)
    dispatch, combine = pl.pallas_call(
        table_kernel,
        in_specs=[in_smem(), in_vmem()],
        out_specs=[in_vmem()] * 2,
        out_shape=[
            jax.ShapeDtypeStruct((far * slots, near * block), jnp.bfloat16),
            jax.ShapeDtypeStruct((near * block, far * slots), jnp.bfloat16),
        ],
        cost_estimate=pl.CostEstimate(
            flops=200_000_000, bytes_accessed=1_200_000, transcendentals=0
        ),
        scratch_shapes=[pltpu.VMEM((near * block, 128), jnp.float32)],
        compiler_params=pltpu.CompilerParams(vmem_limit_bytes=12 << 20),
        name="tables",
    )(jnp.stack([lax.axis_index("head"), lax.axis_index("yp")]), routing)

    outgoing = jnp.dot(dispatch, rows, preferred_element_type=jnp.float32).astype(jnp.bfloat16)
    flat_rows = a2a(outgoing.reshape(far, slots, width), FAR).reshape(far * slots, width)
    tile = 256
    part = w_gate.shape[2]
    partial_value = pl.pallas_call(
        expert_kernel,
        grid=(far * slots // tile,),
        in_specs=[
            pl.BlockSpec((tile, width), lambda i: (i, 0)),
            pl.BlockSpec((part, width), lambda i: (0, 0)),
            pl.BlockSpec((part, width), lambda i: (0, 0)),
            pl.BlockSpec((part, width), lambda i: (0, 0)),
        ],
        out_specs=pl.BlockSpec((tile, width), lambda i: (i, 0)),
        out_shape=pltpu.HBM((far * slots, width), jnp.bfloat16),
        cost_estimate=pl.CostEstimate(
            flops=2_500_000_000, bytes_accessed=11_000_000, transcendentals=200_000
        ),
        compiler_params=pltpu.CompilerParams(vmem_limit_bytes=24 << 20),
        name="experts",
    )(flat_rows, w_gate[0].T, w_up[0].T, w_down[0])
    returned = a2a(partial_value.reshape(far, slots, width), FAR).reshape(far * slots, width)
    columns = 512
    weighted = pl.pallas_call(
        combine_kernel,
        grid=(width // columns,),
        in_specs=[
            pl.BlockSpec((near * block, far * slots), lambda i: (0, 0)),
            pl.BlockSpec((far * slots, columns), lambda i: (0, i)),
        ],
        out_specs=pl.BlockSpec((near * block, columns), lambda i: (0, i)),
        out_shape=jax.ShapeDtypeStruct((near * block, width), jnp.bfloat16),
        cost_estimate=pl.CostEstimate(
            flops=1_100_000_000, bytes_accessed=6_000_000, transcendentals=0
        ),
        compiler_params=pltpu.CompilerParams(vmem_limit_bytes=16 << 20),
        name="combine",
    )(combine, returned)
    parts = a2a(weighted.reshape(near, block, width), BACK)
    moe_out = jnp.sum(parts.astype(jnp.float32), axis=0)
    return (resid + moe_out).astype(jnp.bfloat16)[None]


def solution(mesh):
    fine = Mesh(
        mesh.devices.reshape(2, 4, 4, 2, 2, 4), ("side", "x", "yp", "yq", "zl", "head")
    )
    in_specs = (
        P(STREAM, None, "head"),
        P(STREAM, "head", None, None),
        P(STREAM, "head", None, None),
        P(STREAM, None, "head"),
        P(STREAM, None, "head"),
        P(STREAM),
        P(STREAM, "head", None),
        P("head", "side"),
        P(),
        P(STREAM, "head", None),
        P(STREAM, "head", None),
        P(STREAM, None, "head"),
        P(STREAM, None, "head"),
        P(STREAM, "head", None),
    )
    out_specs = P(STREAM, "head", None)
    return jax.shard_map(shards, mesh=fine, in_specs=in_specs, out_specs=out_specs, check_vma=False)
```

```python
import math

import jax
import jax.numpy as jnp
from jax import lax
from jax.experimental import pallas as pl
from jax.experimental.pallas import tpu as pltpu
from jax.sharding import Mesh
from jax.sharding import PartitionSpec as P

STREAM = ("side", "x", "yp", "yq", "zl")
NEAR = ("head", "yp")
FAR = ("x", "yq", "zl", "side")


def attention_kernel(
    len_ref,
    q_hbm,
    k_hbm,
    v_hbm,
    kn_hbm,
    vn_hbm,
    proj_hbm,
    ctx_ref,
    own_ref,
    q_ref,
    k_ref,
    v_ref,
    kn_ref,
    vn_ref,
    proj_ref,
    sems,
):
    pairs = (
        (q_hbm, q_ref),
        (k_hbm, k_ref),
        (kn_hbm, kn_ref),
        (v_hbm, v_ref),
        (vn_hbm, vn_ref),
        (proj_hbm, proj_ref),
    )
    loads = [
        pltpu.make_async_copy(source, target, sems.at[index])
        for index, (source, target) in enumerate(pairs)
    ]
    for load in loads:
        load.start()
    for load in loads[:-1]:
        load.wait()
    rows = q_ref.shape[1]
    cached, size = k_ref.shape[2], k_ref.shape[3]
    groups = q_ref.shape[2] // size
    per = 2
    scale = 1.0 / math.sqrt(size)
    old_key, new_key = k_ref[0, 0], kn_ref[0]
    old_val, new_val = v_ref[0, 0], vn_ref[0]
    contract = (((1,), (1,)), ((), ()))
    key_pos = lax.broadcasted_iota(jnp.int32, (per * rows, cached), 1)
    old_seen = key_pos < len_ref[0]
    row_pos = lax.broadcasted_iota(jnp.int32, (per * rows, rows), 0) % rows
    new_seen = lax.broadcasted_iota(jnp.int32, (per * rows, rows), 1) <= row_pos
    for start in range(0, groups, per):
        query = jnp.concatenate(
            [q_ref[0, :, (start + g) * size : (start + g + 1) * size] for g in range(per)], axis=0
        )
        old = lax.dot_general(query, old_key, contract, preferred_element_type=jnp.float32) * scale
        new = lax.dot_general(query, new_key, contract, preferred_element_type=jnp.float32) * scale
        old = jnp.where(old_seen, old, -jnp.inf)
        new = jnp.where(new_seen, new, -jnp.inf)
        highest = jnp.maximum(
            jnp.max(old, axis=1, keepdims=True), jnp.max(new, axis=1, keepdims=True)
        )
        old = jnp.exp(old - highest)
        new = jnp.exp(new - highest)
        total = jnp.sum(old, axis=1, keepdims=True) + jnp.sum(new, axis=1, keepdims=True)
        share = 1.0 / total
        context = jnp.dot(
            (old * share).astype(jnp.bfloat16), old_val, preferred_element_type=jnp.float32
        ) + jnp.dot((new * share).astype(jnp.bfloat16), new_val, preferred_element_type=jnp.float32)
        context = context.astype(jnp.bfloat16)
        for g in range(per):
            ctx_ref[:, (start + g) * size : (start + g + 1) * size] = context[
                g * rows : (g + 1) * rows
            ]
    loads[-1].wait()
    own_ref[...] = jnp.dot(
        ctx_ref[...], proj_ref[...], preferred_element_type=jnp.float32
    ).astype(jnp.bfloat16)


def project_kernel(side_ref, ctx_ref, proj_any, own_ref, out_ref, proj_ref, sem):
    load = pltpu.make_async_copy(proj_any, proj_ref, sem)
    load.start()
    load.wait()
    half = proj_ref.shape[1]
    block = out_ref.shape[1]
    side = side_ref[0]
    partner = jnp.dot(
        ctx_ref[...], proj_ref[...], preferred_element_type=jnp.float32
    ).astype(jnp.bfloat16)
    mine = pl.ds(pl.multiple_of(side * half, half), half)
    other = pl.ds(pl.multiple_of((1 - side) * half, half), half)
    for part in range(out_ref.shape[0]):
        take = slice(part * block, (part + 1) * block)
        out_ref[part, :, mine] = own_ref[take]
        out_ref[part, :, other] = partner[take]


def expert_kernel(rows_ref, gate_ref, up_ref, down_ref, out_ref):
    tile = 256
    contract = (((1,), (1,)), ((), ()))

    def step(index, carry):
        take = pl.ds(pl.multiple_of(index * tile, tile), tile)
        rows = rows_ref[take, :]
        gate = lax.dot_general(rows, gate_ref[...], contract, preferred_element_type=jnp.float32)
        up = lax.dot_general(rows, up_ref[...], contract, preferred_element_type=jnp.float32)
        hidden = (gate / (1.0 + jnp.exp(-gate)) * up).astype(jnp.bfloat16)
        out_ref[take, :] = jnp.dot(
            hidden, down_ref[...], preferred_element_type=jnp.float32
        ).astype(jnp.bfloat16)
        return carry

    lax.fori_loop(0, rows_ref.shape[0] // tile, step, 0)


def combine_kernel(combine_ref, rows_ref, out_ref):
    tile = 512

    def step(index, carry):
        take = pl.ds(pl.multiple_of(index * tile, tile), tile)
        out_ref[:, take] = jnp.dot(
            combine_ref[...], rows_ref[:, take], preferred_element_type=jnp.float32
        ).astype(jnp.bfloat16)
        return carry

    lax.fori_loop(0, rows_ref.shape[1] // tile, step, 0)


def in_vmem():
    return pl.BlockSpec(memory_space=pltpu.VMEM)


def in_smem():
    return pl.BlockSpec(memory_space=pltpu.SMEM)


def a2a(value, axes):
    return lax.all_to_all(value, axes, split_axis=0, concat_axis=0, tiled=True)


def dispatch_kernel(part_ref, gathered_ref, out_ref, combine_ref, dispatch_ref):
    top_k, block = 8, 16
    rows, width = gathered_ref.shape[0], gathered_ref.shape[1] - 128
    blocks = rows // block
    columns = jnp.transpose(gathered_ref[:, width:].astype(jnp.float32))
    chosen = columns[:top_k]
    mixing = columns[top_k : 2 * top_k]
    sides, xs, ps, qs, zs = 2, 4, 4, 2, 2
    local = sides * xs * qs * zs
    place = lax.broadcasted_iota(jnp.int32, (local, rows), 0)
    at_z = (place // sides) % zs
    at_q = (place // (sides * zs)) % qs
    at_x = place // (sides * zs * qs)
    expert = (((place % sides) * xs + at_x) * (ps * qs) + part_ref[0] * qs + at_q) * zs + at_z
    expert = expert.astype(jnp.float32)
    named = jnp.zeros((local, rows), jnp.float32)
    weight = jnp.zeros((local, rows), jnp.float32)
    for k in range(top_k):
        hit = chosen[k : k + 1] == expert
        named = jnp.where(hit, 1.0, named)
        weight = jnp.where(hit, mixing[k : k + 1], weight)
    first = lax.broadcasted_iota(jnp.int32, (rows, rows), 0)
    second = lax.broadcasted_iota(jnp.int32, (rows, rows), 1)
    earlier = (first < second) & (first // block == second // block)
    rank = jnp.dot(
        named.astype(jnp.bfloat16),
        jnp.where(earlier, 1.0, 0.0).astype(jnp.bfloat16),
        preferred_element_type=jnp.float32,
    )
    own = lax.broadcasted_iota(jnp.int32, (blocks, rows), 0) == (
        lax.broadcasted_iota(jnp.int32, (blocks, rows), 1) // block
    )
    group = 128 // (2 * blocks)
    for start in range(0, local, group):
        tiles = []
        for e in range(start, start + group):
            for s in range(2):
                takes = (named[e : e + 1] > 0.5) & (jnp.abs(rank[e : e + 1] - s) < 0.5)
                at = (2 * e + s) * blocks
                dispatch_ref[at : at + blocks] = jnp.where(
                    own, jnp.where(takes, 1.0, 0.0), 0.0
                ).astype(jnp.bfloat16)
                tiles.append(jnp.where(own, jnp.where(takes, weight[e : e + 1], 0.0), 0.0))
        at = 2 * start * blocks
        turned = jnp.transpose(jnp.concatenate(tiles, axis=0)).astype(jnp.bfloat16)
        combine_ref[:, at : at + 128] = turned
    tile = 256

    def step(index, carry):
        take = pl.ds(pl.multiple_of(index * tile, tile), tile)
        out_ref[take, :] = jnp.dot(
            dispatch_ref[take, :], gathered_ref[:, :width], preferred_element_type=jnp.float32
        ).astype(jnp.bfloat16)
        return carry

    lax.fori_loop(0, out_ref.shape[0] // tile, step, 0)


def shards(
    q_new,
    k_cache,
    value_cache,
    k_new,
    new_value_rows,
    cache_len,
    hidden_in,
    out_proj,
    norm_gain,
    expert_ids,
    gate_wts,
    w_gate,
    w_up,
    w_down,
):
    width = hidden_in.shape[2]
    block = hidden_in.shape[1]
    side = lax.axis_index("side")
    quarters = lax.axis_size("head")
    near = lax.axis_size(NEAR)
    far = lax.axis_size(FAR)
    slots = 2 * near

    partner_proj = lax.ppermute(out_proj, "side", [(0, 1), (1, 0)])
    half = out_proj.shape[1]
    rows_here = q_new.shape[1]
    context, own = pl.pallas_call(
        attention_kernel,
        in_specs=[in_smem()] + [pl.BlockSpec(memory_space=pltpu.HBM)] * 6,
        out_specs=[in_vmem()] * 2,
        scratch_shapes=[
            pltpu.VMEM(value.shape, jnp.bfloat16)
            for value in (q_new, k_cache, value_cache, k_new, new_value_rows, out_proj)
        ]
        + [pltpu.SemaphoreType.DMA((6,))],
        out_shape=[
            jax.ShapeDtypeStruct((rows_here, q_new.shape[2]), jnp.bfloat16),
            jax.ShapeDtypeStruct((rows_here, half), jnp.bfloat16),
        ],
        cost_estimate=pl.CostEstimate(
            flops=400_000_000, bytes_accessed=3_000_000, transcendentals=300_000
        ),
        compiler_params=pltpu.CompilerParams(vmem_limit_bytes=12 << 20),
        name="attention",
    )(
        cache_len,
        *(
            pltpu.with_memory_space_constraint(value, pltpu.HBM)
            for value in (q_new, k_cache, value_cache, k_new, new_value_rows, out_proj)
        ),
    )
    full_rows = pl.pallas_call(
        project_kernel,
        in_specs=[in_smem(), in_vmem(), pl.BlockSpec(memory_space=pl.ANY), in_vmem()],
        out_specs=in_vmem(),
        scratch_shapes=[pltpu.VMEM(out_proj.shape, jnp.bfloat16), pltpu.SemaphoreType.DMA],
        out_shape=jax.ShapeDtypeStruct((quarters, block, width), jnp.bfloat16),
        cost_estimate=pl.CostEstimate(
            flops=140_000_000, bytes_accessed=2_500_000, transcendentals=0
        ),
        compiler_params=pltpu.CompilerParams(vmem_limit_bytes=12 << 20),
        name="project",
    )(side.reshape(1), context, partner_proj, own)
    pieces = a2a(full_rows, "head")
    resid = hidden_in[0].astype(jnp.float32) + jnp.sum(pieces.astype(jnp.float32), axis=0)
    normed = (
        resid * lax.rsqrt(jnp.mean(resid * resid, axis=-1, keepdims=True) + 1e-06) * norm_gain
    ).astype(jnp.bfloat16)

    raw_wts = gate_wts[0]
    mixing = (raw_wts / jnp.sum(raw_wts, axis=-1, keepdims=True)).astype(jnp.bfloat16)
    routing = jnp.concatenate([expert_ids[0].astype(jnp.bfloat16), mixing], axis=1)
    routing = jnp.pad(routing, ((0, 0), (0, 128 - routing.shape[1])))
    payload = jnp.concatenate([normed, routing], axis=1)
    gathered = a2a(jnp.broadcast_to(payload[None], (near,) + payload.shape), NEAR)
    outgoing, combine = pl.pallas_call(
        dispatch_kernel,
        in_specs=[in_smem(), in_vmem()],
        out_specs=[in_vmem()] * 2,
        out_shape=[
            jax.ShapeDtypeStruct((far * slots, width), jnp.bfloat16),
            jax.ShapeDtypeStruct((near * block, far * slots), jnp.bfloat16),
        ],
        cost_estimate=pl.CostEstimate(
            flops=1_200_000_000, bytes_accessed=6_000_000, transcendentals=0
        ),
        scratch_shapes=[pltpu.VMEM((far * slots, near * block), jnp.bfloat16)],
        compiler_params=pltpu.CompilerParams(vmem_limit_bytes=20 << 20),
        name="dispatch",
    )(lax.axis_index("yp").reshape(1), gathered.reshape(near * block, width + 128))

    flat_rows = a2a(outgoing.reshape(far, slots, width), FAR).reshape(far * slots, width)
    partial_value = pl.pallas_call(
        expert_kernel,
        in_specs=[in_vmem()] * 4,
        out_specs=in_vmem(),
        out_shape=jax.ShapeDtypeStruct((far * slots, width), jnp.bfloat16),
        cost_estimate=pl.CostEstimate(
            flops=2_500_000_000, bytes_accessed=11_000_000, transcendentals=200_000
        ),
        compiler_params=pltpu.CompilerParams(vmem_limit_bytes=24 << 20),
        name="experts",
    )(flat_rows, w_gate[0].T, w_up[0].T, w_down[0])
    returned = a2a(partial_value.reshape(far, slots, width), FAR).reshape(far * slots, width)
    weighted = pl.pallas_call(
        combine_kernel,
        in_specs=[in_vmem()] * 2,
        out_specs=in_vmem(),
        out_shape=jax.ShapeDtypeStruct((near * block, width), jnp.bfloat16),
        cost_estimate=pl.CostEstimate(
            flops=1_100_000_000, bytes_accessed=6_000_000, transcendentals=0
        ),
        compiler_params=pltpu.CompilerParams(vmem_limit_bytes=16 << 20),
        name="combine",
    )(combine, returned)
    parts = a2a(weighted.reshape(near, block, width), NEAR)
    moe_out = jnp.sum(parts.astype(jnp.float32), axis=0)
    return (resid + moe_out).astype(jnp.bfloat16)[None]


def solution(mesh):
    fine = Mesh(
        mesh.devices.reshape(2, 4, 4, 2, 2, 4), ("side", "x", "yp", "yq", "zl", "head")
    )
    in_specs = (
        P(STREAM, None, "head"),
        P(STREAM, "head", None, None),
        P(STREAM, "head", None, None),
        P(STREAM, None, "head"),
        P(STREAM, None, "head"),
        P(STREAM),
        P(STREAM, "head", None),
        P("head", "side"),
        P(),
        P(STREAM, "head", None),
        P(STREAM, "head", None),
        P(STREAM, None, "head"),
        P(STREAM, None, "head"),
        P(STREAM, "head", None),
    )
    out_specs = P(STREAM, "head", None)
    return jax.shard_map(shards, mesh=fine, in_specs=in_specs, out_specs=out_specs, check_vma=False)
```

```python
import math

import jax
import jax.numpy as jnp
from jax import lax
from jax.experimental import pallas as pl
from jax.experimental.pallas import tpu as pltpu
from jax.sharding import Mesh
from jax.sharding import PartitionSpec as P

STREAM = ("side", "x", "yp", "yq", "zl")
NEAR = ("head", "yp")
FAR = ("x", "yq", "zl", "side")


def attention_kernel(
    len_ref,
    q_hbm,
    k_hbm,
    v_hbm,
    kn_hbm,
    vn_hbm,
    proj_hbm,
    ctx_ref,
    own_ref,
    q_ref,
    k_ref,
    v_ref,
    kn_ref,
    vn_ref,
    proj_ref,
    sems,
):
    pairs = (
        (q_hbm, q_ref),
        (k_hbm, k_ref),
        (kn_hbm, kn_ref),
        (v_hbm, v_ref),
        (vn_hbm, vn_ref),
        (proj_hbm, proj_ref),
    )
    loads = [
        pltpu.make_async_copy(source, target, sems.at[index])
        for index, (source, target) in enumerate(pairs)
    ]
    for load in loads:
        load.start()
    for load in loads[:-1]:
        load.wait()
    rows = q_ref.shape[1]
    cached, size = k_ref.shape[2], k_ref.shape[3]
    groups = q_ref.shape[2] // size
    per = 2
    scale = 1.0 / math.sqrt(size)
    old_key, new_key = k_ref[0, 0], kn_ref[0]
    old_val, new_val = v_ref[0, 0], vn_ref[0]
    contract = (((1,), (1,)), ((), ()))
    key_pos = lax.broadcasted_iota(jnp.int32, (per * rows, cached), 1)
    old_seen = key_pos < len_ref[0]
    row_pos = lax.broadcasted_iota(jnp.int32, (per * rows, rows), 0) % rows
    new_seen = lax.broadcasted_iota(jnp.int32, (per * rows, rows), 1) <= row_pos
    for start in range(0, groups, per):
        query = jnp.concatenate(
            [q_ref[0, :, (start + g) * size : (start + g + 1) * size] for g in range(per)], axis=0
        )
        old = lax.dot_general(query, old_key, contract, preferred_element_type=jnp.float32) * scale
        new = lax.dot_general(query, new_key, contract, preferred_element_type=jnp.float32) * scale
        old = jnp.where(old_seen, old, -jnp.inf)
        new = jnp.where(new_seen, new, -jnp.inf)
        highest = jnp.maximum(
            jnp.max(old, axis=1, keepdims=True), jnp.max(new, axis=1, keepdims=True)
        )
        old = jnp.exp(old - highest)
        new = jnp.exp(new - highest)
        total = jnp.sum(old, axis=1, keepdims=True) + jnp.sum(new, axis=1, keepdims=True)
        share = 1.0 / total
        context = jnp.dot(
            (old * share).astype(jnp.bfloat16), old_val, preferred_element_type=jnp.float32
        ) + jnp.dot((new * share).astype(jnp.bfloat16), new_val, preferred_element_type=jnp.float32)
        context = context.astype(jnp.bfloat16)
        for g in range(per):
            ctx_ref[:, (start + g) * size : (start + g + 1) * size] = context[
                g * rows : (g + 1) * rows
            ]
    loads[-1].wait()
    own_ref[...] = jnp.dot(
        ctx_ref[...], proj_ref[...], preferred_element_type=jnp.float32
    ).astype(jnp.bfloat16)


def project_kernel(side_ref, ctx_ref, proj_any, own_ref, out_ref, proj_ref, sem):
    load = pltpu.make_async_copy(proj_any, proj_ref, sem)
    load.start()
    load.wait()
    half = proj_ref.shape[1]
    block = out_ref.shape[1]
    side = side_ref[0]
    partner = jnp.dot(
        ctx_ref[...], proj_ref[...], preferred_element_type=jnp.float32
    ).astype(jnp.bfloat16)
    mine = pl.ds(pl.multiple_of(side * half, half), half)
    other = pl.ds(pl.multiple_of((1 - side) * half, half), half)
    for part in range(out_ref.shape[0]):
        take = slice(part * block, (part + 1) * block)
        out_ref[part, :, mine] = own_ref[take]
        out_ref[part, :, other] = partner[take]


def expert_kernel(rows_ref, gate_ref, up_ref, down_ref, out_ref):
    tile = 256
    contract = (((1,), (1,)), ((), ()))

    def step(index, carry):
        take = pl.ds(pl.multiple_of(index * tile, tile), tile)
        rows = rows_ref[take, :]
        gate = lax.dot_general(rows, gate_ref[...], contract, preferred_element_type=jnp.float32)
        up = lax.dot_general(rows, up_ref[...], contract, preferred_element_type=jnp.float32)
        hidden = (gate / (1.0 + jnp.exp(-gate)) * up).astype(jnp.bfloat16)
        out_ref[take, :] = jnp.dot(
            hidden, down_ref[...], preferred_element_type=jnp.float32
        ).astype(jnp.bfloat16)
        return carry

    lax.fori_loop(0, rows_ref.shape[0] // tile, step, 0)


def combine_kernel(combine_ref, rows_ref, out_ref):
    tile = 512

    def step(index, carry):
        take = pl.ds(pl.multiple_of(index * tile, tile), tile)
        out_ref[:, take] = jnp.dot(
            combine_ref[...], rows_ref[:, take], preferred_element_type=jnp.float32
        ).astype(jnp.bfloat16)
        return carry

    lax.fori_loop(0, rows_ref.shape[1] // tile, step, 0)


def in_vmem():
    return pl.BlockSpec(memory_space=pltpu.VMEM)


def in_smem():
    return pl.BlockSpec(memory_space=pltpu.SMEM)


def a2a(value, axes):
    return lax.all_to_all(value, axes, split_axis=0, concat_axis=0, tiled=True)


def norm_kernel(pieces_ref, hidden_ref, gain_ref, routing_ref, resid_ref, out_ref, row_ref, sems):
    width = hidden_ref.shape[2]
    resid = hidden_ref[0].astype(jnp.float32)
    resid = resid + jnp.sum(pieces_ref[...].astype(jnp.float32), axis=0)
    resid_ref[...] = resid
    mean = jnp.mean(resid * resid, axis=1, keepdims=True)
    row_ref[:, :width] = (resid * lax.rsqrt(mean + 1e-06) * gain_ref[...]).astype(jnp.bfloat16)
    row_ref[:, width:] = routing_ref[...]
    copies = [
        pltpu.make_async_copy(row_ref, out_ref.at[peer], sems.at[peer])
        for peer in range(out_ref.shape[0])
    ]
    for copy in copies:
        copy.start()
    for copy in copies:
        copy.wait()


def dispatch_kernel(part_ref, gathered_ref, out_ref, combine_ref, dispatch_ref):
    top_k, block = 8, 16
    rows, width = gathered_ref.shape[0], gathered_ref.shape[1] - 128
    blocks = rows // block
    columns = jnp.transpose(gathered_ref[:, width:].astype(jnp.float32))
    chosen = columns[:top_k]
    mixing = columns[top_k : 2 * top_k]
    sides, xs, ps, qs, zs = 2, 4, 4, 2, 2
    local = sides * xs * qs * zs
    place = lax.broadcasted_iota(jnp.int32, (local, rows), 0)
    at_z = (place // sides) % zs
    at_q = (place // (sides * zs)) % qs
    at_x = place // (sides * zs * qs)
    expert = (((place % sides) * xs + at_x) * (ps * qs) + part_ref[0] * qs + at_q) * zs + at_z
    expert = expert.astype(jnp.float32)
    named = jnp.zeros((local, rows), jnp.float32)
    weight = jnp.zeros((local, rows), jnp.float32)
    for k in range(top_k):
        hit = chosen[k : k + 1] == expert
        named = jnp.where(hit, 1.0, named)
        weight = jnp.where(hit, mixing[k : k + 1], weight)
    first = lax.broadcasted_iota(jnp.int32, (rows, rows), 0)
    second = lax.broadcasted_iota(jnp.int32, (rows, rows), 1)
    earlier = (first < second) & (first // block == second // block)
    rank = jnp.dot(
        named.astype(jnp.bfloat16),
        jnp.where(earlier, 1.0, 0.0).astype(jnp.bfloat16),
        preferred_element_type=jnp.float32,
    )
    own = lax.broadcasted_iota(jnp.int32, (blocks, rows), 0) == (
        lax.broadcasted_iota(jnp.int32, (blocks, rows), 1) // block
    )
    group = 128 // (2 * blocks)
    for start in range(0, local, group):
        tiles = []
        for e in range(start, start + group):
            for s in range(2):
                takes = (named[e : e + 1] > 0.5) & (jnp.abs(rank[e : e + 1] - s) < 0.5)
                at = (2 * e + s) * blocks
                dispatch_ref[at : at + blocks] = jnp.where(
                    own, jnp.where(takes, 1.0, 0.0), 0.0
                ).astype(jnp.bfloat16)
                tiles.append(jnp.where(own, jnp.where(takes, weight[e : e + 1], 0.0), 0.0))
        at = 2 * start * blocks
        turned = jnp.transpose(jnp.concatenate(tiles, axis=0)).astype(jnp.bfloat16)
        combine_ref[:, at : at + 128] = turned
    tile = 256

    def step(index, carry):
        take = pl.ds(pl.multiple_of(index * tile, tile), tile)
        out_ref[take, :] = jnp.dot(
            dispatch_ref[take, :], gathered_ref[:, :width], preferred_element_type=jnp.float32
        ).astype(jnp.bfloat16)
        return carry

    lax.fori_loop(0, out_ref.shape[0] // tile, step, 0)


def shards(
    q_new,
    k_cache,
    value_cache,
    k_new,
    new_value_rows,
    cache_len,
    hidden_in,
    out_proj,
    norm_gain,
    expert_ids,
    gate_wts,
    w_gate,
    w_up,
    w_down,
):
    width = hidden_in.shape[2]
    block = hidden_in.shape[1]
    side = lax.axis_index("side")
    quarters = lax.axis_size("head")
    near = lax.axis_size(NEAR)
    far = lax.axis_size(FAR)
    slots = 2 * near

    partner_proj = lax.ppermute(out_proj, "side", [(0, 1), (1, 0)])
    half = out_proj.shape[1]
    rows_here = q_new.shape[1]
    context, own = pl.pallas_call(
        attention_kernel,
        in_specs=[in_smem()] + [pl.BlockSpec(memory_space=pltpu.HBM)] * 6,
        out_specs=[in_vmem()] * 2,
        scratch_shapes=[
            pltpu.VMEM(value.shape, jnp.bfloat16)
            for value in (q_new, k_cache, value_cache, k_new, new_value_rows, out_proj)
        ]
        + [pltpu.SemaphoreType.DMA((6,))],
        out_shape=[
            jax.ShapeDtypeStruct((rows_here, q_new.shape[2]), jnp.bfloat16),
            jax.ShapeDtypeStruct((rows_here, half), jnp.bfloat16),
        ],
        cost_estimate=pl.CostEstimate(
            flops=400_000_000, bytes_accessed=3_000_000, transcendentals=300_000
        ),
        compiler_params=pltpu.CompilerParams(vmem_limit_bytes=12 << 20),
        name="attention",
    )(
        cache_len,
        *(
            pltpu.with_memory_space_constraint(value, pltpu.HBM)
            for value in (q_new, k_cache, value_cache, k_new, new_value_rows, out_proj)
        ),
    )
    full_rows = pl.pallas_call(
        project_kernel,
        in_specs=[in_smem(), in_vmem(), pl.BlockSpec(memory_space=pl.ANY), in_vmem()],
        out_specs=in_vmem(),
        scratch_shapes=[pltpu.VMEM(out_proj.shape, jnp.bfloat16), pltpu.SemaphoreType.DMA],
        out_shape=jax.ShapeDtypeStruct((quarters, block, width), jnp.bfloat16),
        cost_estimate=pl.CostEstimate(
            flops=140_000_000, bytes_accessed=2_500_000, transcendentals=0
        ),
        compiler_params=pltpu.CompilerParams(vmem_limit_bytes=12 << 20),
        name="project",
    )(side.reshape(1), context, partner_proj, own)
    pieces = a2a(full_rows, "head")
    raw_wts = gate_wts[0]
    mixing = (raw_wts / jnp.sum(raw_wts, axis=-1, keepdims=True)).astype(jnp.bfloat16)
    routing = jnp.concatenate([expert_ids[0].astype(jnp.bfloat16), mixing], axis=1)
    routing = jnp.pad(routing, ((0, 0), (0, 128 - routing.shape[1])))
    resid, payload = pl.pallas_call(
        norm_kernel,
        in_specs=[in_vmem()] * 4,
        out_specs=[in_vmem(), pl.BlockSpec(memory_space=pltpu.HBM)],
        out_shape=[
            jax.ShapeDtypeStruct((block, width), jnp.float32),
            jax.ShapeDtypeStruct((near, block, width + 128), jnp.bfloat16),
        ],
        scratch_shapes=[
            pltpu.VMEM((block, width + 128), jnp.bfloat16),
            pltpu.SemaphoreType.DMA((near,)),
        ],
        cost_estimate=pl.CostEstimate(flops=500_000, bytes_accessed=1_500_000, transcendentals=0),
        compiler_params=pltpu.CompilerParams(vmem_limit_bytes=8 << 20),
        name="norm",
    )(pieces, hidden_in, norm_gain.reshape(1, width), routing)
    gathered = a2a(payload, NEAR)
    outgoing, combine = pl.pallas_call(
        dispatch_kernel,
        in_specs=[in_smem(), in_vmem()],
        out_specs=[in_vmem()] * 2,
        out_shape=[
            jax.ShapeDtypeStruct((far * slots, width), jnp.bfloat16),
            jax.ShapeDtypeStruct((near * block, far * slots), jnp.bfloat16),
        ],
        cost_estimate=pl.CostEstimate(
            flops=1_200_000_000, bytes_accessed=6_000_000, transcendentals=0
        ),
        scratch_shapes=[pltpu.VMEM((far * slots, near * block), jnp.bfloat16)],
        compiler_params=pltpu.CompilerParams(vmem_limit_bytes=20 << 20),
        name="dispatch",
    )(lax.axis_index("yp").reshape(1), gathered.reshape(near * block, width + 128))

    flat_rows = a2a(outgoing.reshape(far, slots, width), FAR).reshape(far * slots, width)
    partial_value = pl.pallas_call(
        expert_kernel,
        in_specs=[in_vmem()] * 4,
        out_specs=in_vmem(),
        out_shape=jax.ShapeDtypeStruct((far * slots, width), jnp.bfloat16),
        cost_estimate=pl.CostEstimate(
            flops=2_500_000_000, bytes_accessed=11_000_000, transcendentals=200_000
        ),
        compiler_params=pltpu.CompilerParams(vmem_limit_bytes=24 << 20),
        name="experts",
    )(flat_rows, w_gate[0].T, w_up[0].T, w_down[0])
    returned = a2a(partial_value.reshape(far, slots, width), FAR).reshape(far * slots, width)
    weighted = pl.pallas_call(
        combine_kernel,
        in_specs=[in_vmem()] * 2,
        out_specs=in_vmem(),
        out_shape=jax.ShapeDtypeStruct((near * block, width), jnp.bfloat16),
        cost_estimate=pl.CostEstimate(
            flops=1_100_000_000, bytes_accessed=6_000_000, transcendentals=0
        ),
        compiler_params=pltpu.CompilerParams(vmem_limit_bytes=16 << 20),
        name="combine",
    )(combine, returned)
    parts = a2a(weighted.reshape(near, block, width), NEAR)
    moe_out = jnp.sum(parts.astype(jnp.float32), axis=0)
    return (resid + moe_out).astype(jnp.bfloat16)[None]


def solution(mesh):
    fine = Mesh(
        mesh.devices.reshape(2, 4, 4, 2, 2, 4), ("side", "x", "yp", "yq", "zl", "head")
    )
    in_specs = (
        P(STREAM, None, "head"),
        P(STREAM, "head", None, None),
        P(STREAM, "head", None, None),
        P(STREAM, None, "head"),
        P(STREAM, None, "head"),
        P(STREAM),
        P(STREAM, "head", None),
        P("head", "side"),
        P(),
        P(STREAM, "head", None),
        P(STREAM, "head", None),
        P(STREAM, None, "head"),
        P(STREAM, None, "head"),
        P(STREAM, "head", None),
    )
    out_specs = P(STREAM, "head", None)
    return jax.shard_map(shards, mesh=fine, in_specs=in_specs, out_specs=out_specs, check_vma=False)
```

```python
import functools
import math

import jax
import jax.numpy as jnp
from jax import lax
from jax.experimental import pallas as pl
from jax.experimental.pallas import tpu as pltpu
from jax.sharding import Mesh
from jax.sharding import PartitionSpec as P

STREAM = ("side", "x", "yp", "yq", "zl")
NEAR = ("head", "yp")
FAR = ("x", "yq", "zl", "side")


def attention_kernel(
    len_ref,
    q_hbm,
    k_hbm,
    v_hbm,
    kn_hbm,
    vn_hbm,
    proj_hbm,
    ctx_ref,
    own_ref,
    q_ref,
    k_ref,
    v_ref,
    kn_ref,
    vn_ref,
    proj_ref,
    sems,
):
    pairs = (
        (q_hbm, q_ref),
        (k_hbm, k_ref),
        (kn_hbm, kn_ref),
        (v_hbm, v_ref),
        (vn_hbm, vn_ref),
        (proj_hbm, proj_ref),
    )
    loads = [
        pltpu.make_async_copy(source, target, sems.at[index])
        for index, (source, target) in enumerate(pairs)
    ]
    for load in loads:
        load.start()
    for load in loads[:-1]:
        load.wait()
    rows = q_ref.shape[1]
    cached, size = k_ref.shape[2], k_ref.shape[3]
    groups = q_ref.shape[2] // size
    per = 2
    scale = 1.0 / math.sqrt(size)
    old_key, new_key = k_ref[0, 0], kn_ref[0]
    old_val, new_val = v_ref[0, 0], vn_ref[0]
    contract = (((1,), (1,)), ((), ()))
    key_pos = lax.broadcasted_iota(jnp.int32, (per * rows, cached), 1)
    old_seen = key_pos < len_ref[0]
    row_pos = lax.broadcasted_iota(jnp.int32, (per * rows, rows), 0) % rows
    new_seen = lax.broadcasted_iota(jnp.int32, (per * rows, rows), 1) <= row_pos
    for start in range(0, groups, per):
        query = jnp.concatenate(
            [q_ref[0, :, (start + g) * size : (start + g + 1) * size] for g in range(per)], axis=0
        )
        old = lax.dot_general(query, old_key, contract, preferred_element_type=jnp.float32) * scale
        new = lax.dot_general(query, new_key, contract, preferred_element_type=jnp.float32) * scale
        old = jnp.where(old_seen, old, -jnp.inf)
        new = jnp.where(new_seen, new, -jnp.inf)
        highest = jnp.maximum(
            jnp.max(old, axis=1, keepdims=True), jnp.max(new, axis=1, keepdims=True)
        )
        old = jnp.exp(old - highest)
        new = jnp.exp(new - highest)
        total = jnp.sum(old, axis=1, keepdims=True) + jnp.sum(new, axis=1, keepdims=True)
        share = 1.0 / total
        context = jnp.dot(
            (old * share).astype(jnp.bfloat16), old_val, preferred_element_type=jnp.float32
        ) + jnp.dot((new * share).astype(jnp.bfloat16), new_val, preferred_element_type=jnp.float32)
        context = context.astype(jnp.bfloat16)
        for g in range(per):
            ctx_ref[:, (start + g) * size : (start + g + 1) * size] = context[
                g * rows : (g + 1) * rows
            ]
    loads[-1].wait()
    own_ref[...] = jnp.dot(
        ctx_ref[...], proj_ref[...], preferred_element_type=jnp.float32
    ).astype(jnp.bfloat16)


def project_kernel(side_ref, ctx_ref, proj_any, own_ref, out_ref, proj_ref, sem):
    load = pltpu.make_async_copy(proj_any, proj_ref, sem)
    load.start()
    load.wait()
    half = proj_ref.shape[1]
    block = out_ref.shape[1]
    side = side_ref[0]
    partner = jnp.dot(
        ctx_ref[...], proj_ref[...], preferred_element_type=jnp.float32
    ).astype(jnp.bfloat16)
    mine = pl.ds(pl.multiple_of(side * half, half), half)
    other = pl.ds(pl.multiple_of((1 - side) * half, half), half)
    for part in range(out_ref.shape[0]):
        take = slice(part * block, (part + 1) * block)
        out_ref[part, :, mine] = own_ref[take]
        out_ref[part, :, other] = partner[take]


def fetch_tiles(source_hbm, target_ref, sems, tiles):
    tile = source_hbm.shape[0] // tiles
    loads = [
        pltpu.make_async_copy(
            source_hbm.at[pl.ds(index * tile, tile)],
            target_ref.at[pl.ds(index * tile, tile)],
            sems.at[index],
        )
        for index in range(tiles)
    ]
    for load in loads:
        load.start()
    return loads


def expert_kernel(
    rows_hbm, gate_ref, up_ref, down_hbm, out_hbm, rows_ref, down_ref, in_sems, stage_ref, sems
):
    contract = (((1,), (1,)), ((), ()))
    tiles = rows_hbm.shape[0] // stage_ref.shape[1]
    loads = fetch_tiles(rows_hbm, rows_ref, in_sems, tiles)
    down_load = pltpu.make_async_copy(down_hbm, down_ref, in_sems.at[tiles])
    down_load.start()

    def make(start, tile):
        loads[start // tile].wait()
        rows = rows_ref[start : start + tile]
        gate = lax.dot_general(rows, gate_ref[...], contract, preferred_element_type=jnp.float32)
        up = lax.dot_general(rows, up_ref[...], contract, preferred_element_type=jnp.float32)
        hidden = (gate / (1.0 + jnp.exp(-gate)) * up).astype(jnp.bfloat16)
        if start == 0:
            down_load.wait()
        return jnp.dot(hidden, down_ref[...], preferred_element_type=jnp.float32).astype(
            jnp.bfloat16
        )

    send_tiles(make, out_hbm, stage_ref, sems)


def combine_kernel(first_ref, second_ref, rows_hbm, out_ref, rows_ref, total_ref, sems):
    half = first_ref.shape[1]
    tiles = sems.shape[0]
    tile = rows_hbm.shape[0] // tiles
    loads = fetch_tiles(rows_hbm, rows_ref, sems, tiles)
    for index, load in enumerate(loads):
        load.wait()
        start = index * tile
        table = first_ref if start < half else second_ref
        product = jnp.dot(
            table[:, start % half : start % half + tile],
            rows_ref[start : start + tile],
            preferred_element_type=jnp.float32,
        )
        if index == 0:
            total_ref[...] = product
        elif index < tiles - 1:
            total_ref[...] += product
        else:
            out_ref[...] = (total_ref[...] + product).astype(jnp.bfloat16)


def in_vmem():
    return pl.BlockSpec(memory_space=pltpu.VMEM)


def in_smem():
    return pl.BlockSpec(memory_space=pltpu.SMEM)


def a2a(value, axes):
    return lax.all_to_all(value, axes, split_axis=0, concat_axis=0, tiled=True)


def norm_kernel(pieces_ref, hidden_ref, gain_ref, routing_ref, resid_ref, out_ref, row_ref, sems):
    width = hidden_ref.shape[2]
    resid = hidden_ref[0].astype(jnp.float32)
    resid = resid + jnp.sum(pieces_ref[...].astype(jnp.float32), axis=0)
    resid_ref[...] = resid
    mean = jnp.mean(resid * resid, axis=1, keepdims=True)
    row_ref[:, :width] = (resid * lax.rsqrt(mean + 1e-06) * gain_ref[...]).astype(jnp.bfloat16)
    row_ref[:, width:] = routing_ref[...]
    copies = [
        pltpu.make_async_copy(row_ref, out_ref.at[peer], sems.at[peer])
        for peer in range(out_ref.shape[0])
    ]
    for copy in copies:
        copy.start()
    for copy in copies:
        copy.wait()


def routed(part_ref, gathered_ref):
    top_k, block = 8, 16
    rows, width = gathered_ref.shape[0], gathered_ref.shape[1] - 128
    columns = jnp.transpose(gathered_ref[:, width:].astype(jnp.float32))
    chosen = columns[:top_k]
    mixing = columns[top_k : 2 * top_k]
    sides, xs, ps, qs, zs = 2, 4, 4, 2, 2
    local = sides * xs * qs * zs
    place = lax.broadcasted_iota(jnp.int32, (local, rows), 0)
    at_z = (place // sides) % zs
    at_q = (place // (sides * zs)) % qs
    at_x = place // (sides * zs * qs)
    expert = (((place % sides) * xs + at_x) * (ps * qs) + part_ref[0] * qs + at_q) * zs + at_z
    expert = expert.astype(jnp.float32)
    named = jnp.zeros((local, rows), jnp.float32)
    weight = jnp.zeros((local, rows), jnp.float32)
    for k in range(top_k):
        hit = chosen[k : k + 1] == expert
        named = jnp.where(hit, 1.0, named)
        weight = jnp.where(hit, mixing[k : k + 1], weight)
    first = lax.broadcasted_iota(jnp.int32, (rows, rows), 0)
    second = lax.broadcasted_iota(jnp.int32, (rows, rows), 1)
    earlier = (first < second) & (first // block == second // block)
    rank = jnp.dot(
        named.astype(jnp.bfloat16),
        jnp.where(earlier, 1.0, 0.0).astype(jnp.bfloat16),
        preferred_element_type=jnp.float32,
    )
    blocks = rows // block
    own = lax.broadcasted_iota(jnp.int32, (blocks, rows), 0) == (
        lax.broadcasted_iota(jnp.int32, (blocks, rows), 1) // block
    )
    return named, rank, weight, own


def send_tiles(make, out_hbm, stage_ref, sems):
    slots, tile = stage_ref.shape[0], stage_ref.shape[1]
    copies = []
    for index in range(out_hbm.shape[0] // tile):
        slot = index % slots
        if index >= slots:
            copies[index - slots].wait()
        stage_ref[slot] = make(index * tile, tile)
        copy = pltpu.make_async_copy(
            stage_ref.at[slot], out_hbm.at[pl.ds(index * tile, tile)], sems.at[slot]
        )
        copy.start()
        copies.append(copy)
    for copy in copies[-slots:]:
        copy.wait()


def dispatch_kernel(part_ref, gathered_ref, out_hbm, dispatch_ref, stage_ref, sems):
    width = gathered_ref.shape[1] - 128
    named, rank, _, own = routed(part_ref, gathered_ref)
    blocks = own.shape[0]
    for e in range(named.shape[0]):
        for s in range(2):
            takes = (named[e : e + 1] > 0.5) & (jnp.abs(rank[e : e + 1] - s) < 0.5)
            at = (2 * e + s) * blocks
            dispatch_ref[at : at + blocks] = jnp.where(
                own, jnp.where(takes, 1.0, 0.0), 0.0
            ).astype(jnp.bfloat16)

    def make(start, tile):
        return jnp.dot(
            dispatch_ref[start : start + tile],
            gathered_ref[:, :width],
            preferred_element_type=jnp.float32,
        ).astype(jnp.bfloat16)

    send_tiles(make, out_hbm, stage_ref, sems)


def weight_kernel(begin, part_ref, gathered_ref, combine_ref):
    named, rank, weight, own = routed(part_ref, gathered_ref)
    blocks = own.shape[0]
    group = 128 // (2 * blocks)
    for start in range(0, named.shape[0] // 2, group):
        tiles = []
        for e in range(begin + start, begin + start + group):
            for s in range(2):
                takes = (named[e : e + 1] > 0.5) & (jnp.abs(rank[e : e + 1] - s) < 0.5)
                tiles.append(jnp.where(own, jnp.where(takes, weight[e : e + 1], 0.0), 0.0))
        at = 2 * start * blocks
        combine_ref[:, at : at + 128] = jnp.transpose(jnp.concatenate(tiles, axis=0)).astype(
            jnp.bfloat16
        )


def shards(
    q_new,
    k_cache,
    value_cache,
    k_new,
    new_value_rows,
    cache_len,
    hidden_in,
    out_proj,
    norm_gain,
    expert_ids,
    gate_wts,
    w_gate,
    w_up,
    w_down,
):
    width = hidden_in.shape[2]
    block = hidden_in.shape[1]
    side = lax.axis_index("side")
    quarters = lax.axis_size("head")
    near = lax.axis_size(NEAR)
    far = lax.axis_size(FAR)
    slots = 2 * near

    partner_proj = lax.ppermute(out_proj, "side", [(0, 1), (1, 0)])
    half = out_proj.shape[1]
    rows_here = q_new.shape[1]
    context, own = pl.pallas_call(
        attention_kernel,
        in_specs=[in_smem()] + [pl.BlockSpec(memory_space=pltpu.HBM)] * 6,
        out_specs=[in_vmem()] * 2,
        scratch_shapes=[
            pltpu.VMEM(value.shape, jnp.bfloat16)
            for value in (q_new, k_cache, value_cache, k_new, new_value_rows, out_proj)
        ]
        + [pltpu.SemaphoreType.DMA((6,))],
        out_shape=[
            jax.ShapeDtypeStruct((rows_here, q_new.shape[2]), jnp.bfloat16),
            jax.ShapeDtypeStruct((rows_here, half), jnp.bfloat16),
        ],
        cost_estimate=pl.CostEstimate(
            flops=400_000_000, bytes_accessed=3_000_000, transcendentals=300_000
        ),
        compiler_params=pltpu.CompilerParams(vmem_limit_bytes=12 << 20),
        name="attention",
    )(
        cache_len,
        *(
            pltpu.with_memory_space_constraint(value, pltpu.HBM)
            for value in (q_new, k_cache, value_cache, k_new, new_value_rows, out_proj)
        ),
    )
    full_rows = pl.pallas_call(
        project_kernel,
        in_specs=[in_smem(), in_vmem(), pl.BlockSpec(memory_space=pl.ANY), in_vmem()],
        out_specs=in_vmem(),
        scratch_shapes=[pltpu.VMEM(out_proj.shape, jnp.bfloat16), pltpu.SemaphoreType.DMA],
        out_shape=jax.ShapeDtypeStruct((quarters, block, width), jnp.bfloat16),
        cost_estimate=pl.CostEstimate(
            flops=140_000_000, bytes_accessed=2_500_000, transcendentals=0
        ),
        compiler_params=pltpu.CompilerParams(vmem_limit_bytes=12 << 20),
        name="project",
    )(side.reshape(1), context, partner_proj, own)
    pieces = a2a(full_rows, "head")
    raw_wts = gate_wts[0]
    mixing = (raw_wts / jnp.sum(raw_wts, axis=-1, keepdims=True)).astype(jnp.bfloat16)
    routing = jnp.concatenate([expert_ids[0].astype(jnp.bfloat16), mixing], axis=1)
    routing = jnp.pad(routing, ((0, 0), (0, 128 - routing.shape[1])))
    resid, payload = pl.pallas_call(
        norm_kernel,
        in_specs=[in_vmem()] * 4,
        out_specs=[in_vmem(), pl.BlockSpec(memory_space=pltpu.HBM)],
        out_shape=[
            jax.ShapeDtypeStruct((block, width), jnp.float32),
            jax.ShapeDtypeStruct((near, block, width + 128), jnp.bfloat16),
        ],
        scratch_shapes=[
            pltpu.VMEM((block, width + 128), jnp.bfloat16),
            pltpu.SemaphoreType.DMA((near,)),
        ],
        cost_estimate=pl.CostEstimate(flops=500_000, bytes_accessed=1_500_000, transcendentals=0),
        compiler_params=pltpu.CompilerParams(vmem_limit_bytes=8 << 20),
        name="norm",
    )(pieces, hidden_in, norm_gain.reshape(1, width), routing)
    gathered = a2a(payload, NEAR)
    gathered = gathered.reshape(near * block, width + 128)
    part = lax.axis_index("yp").reshape(1)
    tile = 256
    staging = [pltpu.VMEM((2, tile, width), jnp.bfloat16), pltpu.SemaphoreType.DMA((2,))]
    slot_rows = pltpu.HBM((far * slots, width), jnp.bfloat16)
    outgoing = pl.pallas_call(
        dispatch_kernel,
        in_specs=[in_smem(), in_vmem()],
        out_specs=pl.BlockSpec(memory_space=pltpu.HBM),
        out_shape=slot_rows,
        cost_estimate=pl.CostEstimate(
            flops=1_200_000_000, bytes_accessed=6_000_000, transcendentals=0
        ),
        scratch_shapes=[pltpu.VMEM((far * slots, near * block), jnp.bfloat16)] + staging,
        compiler_params=pltpu.CompilerParams(vmem_limit_bytes=20 << 20),
        name="dispatch",
    )(part, gathered)

    def weights_of(begin, rows):
        return pl.pallas_call(
            functools.partial(weight_kernel, begin),
            in_specs=[in_smem(), in_vmem()],
            out_specs=in_vmem(),
            out_shape=jax.ShapeDtypeStruct((near * block, far * slots // 2), jnp.bfloat16),
            cost_estimate=pl.CostEstimate(
                flops=200_000_000, bytes_accessed=1_200_000, transcendentals=0
            ),
            compiler_params=pltpu.CompilerParams(vmem_limit_bytes=12 << 20),
            name="weights",
        )(part, rows)

    outgoing, gathered = lax.optimization_barrier((outgoing, gathered))
    first_weights = weights_of(0, gathered)
    flat_rows = a2a(outgoing.reshape(far, slots, width), FAR).reshape(far * slots, width)
    flat_rows, first_weights = lax.optimization_barrier((flat_rows, first_weights))
    partial_value = pl.pallas_call(
        expert_kernel,
        in_specs=[pl.BlockSpec(memory_space=pl.ANY)]
        + [in_vmem()] * 2
        + [pl.BlockSpec(memory_space=pltpu.HBM)],
        out_specs=pl.BlockSpec(memory_space=pltpu.HBM),
        out_shape=slot_rows,
        scratch_shapes=[
            pltpu.VMEM((far * slots, width), jnp.bfloat16),
            pltpu.VMEM(w_down.shape[1:], jnp.bfloat16),
            pltpu.SemaphoreType.DMA((far * slots // tile + 1,)),
        ]
        + staging,
        cost_estimate=pl.CostEstimate(
            flops=2_500_000_000, bytes_accessed=11_000_000, transcendentals=200_000
        ),
        compiler_params=pltpu.CompilerParams(vmem_limit_bytes=24 << 20),
        name="experts",
    )(
        flat_rows,
        w_gate[0].T,
        w_up[0].T,
        pltpu.with_memory_space_constraint(w_down[0], pltpu.HBM),
    )
    partial_value, gathered = lax.optimization_barrier((partial_value, gathered))
    second_weights = weights_of(far // 2, gathered)
    returned = a2a(partial_value.reshape(far, slots, width), FAR).reshape(far * slots, width)
    weighted = pl.pallas_call(
        combine_kernel,
        in_specs=[in_vmem()] * 2 + [pl.BlockSpec(memory_space=pl.ANY)],
        out_specs=in_vmem(),
        scratch_shapes=[
            pltpu.VMEM((far * slots, width), jnp.bfloat16),
            pltpu.VMEM((near * block, width), jnp.float32),
            pltpu.SemaphoreType.DMA((far * slots // tile,)),
        ],
        out_shape=jax.ShapeDtypeStruct((near * block, width), jnp.bfloat16),
        cost_estimate=pl.CostEstimate(
            flops=1_100_000_000, bytes_accessed=6_000_000, transcendentals=0
        ),
        compiler_params=pltpu.CompilerParams(vmem_limit_bytes=16 << 20),
        name="combine",
    )(first_weights, second_weights, returned)
    parts = a2a(weighted.reshape(near, block, width), NEAR)
    moe_out = jnp.sum(parts.astype(jnp.float32), axis=0)
    return (resid + moe_out).astype(jnp.bfloat16)[None]


def solution(mesh):
    fine = Mesh(
        mesh.devices.reshape(2, 4, 4, 2, 2, 4), ("side", "x", "yp", "yq", "zl", "head")
    )
    in_specs = (
        P(STREAM, None, "head"),
        P(STREAM, "head", None, None),
        P(STREAM, "head", None, None),
        P(STREAM, None, "head"),
        P(STREAM, None, "head"),
        P(STREAM),
        P(STREAM, "head", None),
        P("head", "side"),
        P(),
        P(STREAM, "head", None),
        P(STREAM, "head", None),
        P(STREAM, None, "head"),
        P(STREAM, None, "head"),
        P(STREAM, "head", None),
    )
    out_specs = P(STREAM, "head", None)
    return jax.shard_map(shards, mesh=fine, in_specs=in_specs, out_specs=out_specs, check_vma=False)
```

```python
import math

import jax
import jax.numpy as jnp
from jax import lax
from jax.experimental import pallas as pl
from jax.experimental.pallas import tpu as pltpu
from jax.sharding import Mesh
from jax.sharding import PartitionSpec as P

STREAM = ("side", "x", "yp", "yq", "zl")
NEAR = ("head", "yp")
FAR = ("x", "yq", "zl", "side")


def attention_kernel(
    len_ref,
    q_hbm,
    k_hbm,
    v_hbm,
    kn_hbm,
    vn_hbm,
    proj_hbm,
    ctx_ref,
    own_ref,
    q_ref,
    k_ref,
    v_ref,
    kn_ref,
    vn_ref,
    proj_ref,
    sems,
):
    pairs = (
        (q_hbm, q_ref),
        (k_hbm, k_ref),
        (kn_hbm, kn_ref),
        (v_hbm, v_ref),
        (vn_hbm, vn_ref),
        (proj_hbm, proj_ref),
    )
    loads = [
        pltpu.make_async_copy(source, target, sems.at[index])
        for index, (source, target) in enumerate(pairs)
    ]
    for load in loads:
        load.start()
    for load in loads[:-1]:
        load.wait()
    rows = q_ref.shape[1]
    cached, size = k_ref.shape[2], k_ref.shape[3]
    groups = q_ref.shape[2] // size
    per = 2
    scale = 1.0 / math.sqrt(size)
    old_key, new_key = k_ref[0, 0], kn_ref[0]
    old_val, new_val = v_ref[0, 0], vn_ref[0]
    contract = (((1,), (1,)), ((), ()))
    key_pos = lax.broadcasted_iota(jnp.int32, (per * rows, cached), 1)
    old_seen = key_pos < len_ref[0]
    row_pos = lax.broadcasted_iota(jnp.int32, (per * rows, rows), 0) % rows
    new_seen = lax.broadcasted_iota(jnp.int32, (per * rows, rows), 1) <= row_pos
    for start in range(0, groups, per):
        query = jnp.concatenate(
            [q_ref[0, :, (start + g) * size : (start + g + 1) * size] for g in range(per)], axis=0
        )
        old = lax.dot_general(query, old_key, contract, preferred_element_type=jnp.float32) * scale
        new = lax.dot_general(query, new_key, contract, preferred_element_type=jnp.float32) * scale
        old = jnp.where(old_seen, old, -jnp.inf)
        new = jnp.where(new_seen, new, -jnp.inf)
        highest = jnp.maximum(
            jnp.max(old, axis=1, keepdims=True), jnp.max(new, axis=1, keepdims=True)
        )
        old = jnp.exp(old - highest)
        new = jnp.exp(new - highest)
        total = jnp.sum(old, axis=1, keepdims=True) + jnp.sum(new, axis=1, keepdims=True)
        share = 1.0 / total
        context = jnp.dot(
            (old * share).astype(jnp.bfloat16), old_val, preferred_element_type=jnp.float32
        ) + jnp.dot((new * share).astype(jnp.bfloat16), new_val, preferred_element_type=jnp.float32)
        context = context.astype(jnp.bfloat16)
        for g in range(per):
            ctx_ref[:, (start + g) * size : (start + g + 1) * size] = context[
                g * rows : (g + 1) * rows
            ]
    loads[-1].wait()
    own_ref[...] = jnp.dot(
        ctx_ref[...], proj_ref[...], preferred_element_type=jnp.float32
    ).astype(jnp.bfloat16)


def project_kernel(side_ref, ctx_ref, proj_any, own_ref, out_ref, proj_ref, sem):
    load = pltpu.make_async_copy(proj_any, proj_ref, sem)
    load.start()
    load.wait()
    half = proj_ref.shape[1]
    block = out_ref.shape[1]
    side = side_ref[0]
    partner = jnp.dot(
        ctx_ref[...], proj_ref[...], preferred_element_type=jnp.float32
    ).astype(jnp.bfloat16)
    mine = pl.ds(pl.multiple_of(side * half, half), half)
    other = pl.ds(pl.multiple_of((1 - side) * half, half), half)
    for part in range(out_ref.shape[0]):
        take = slice(part * block, (part + 1) * block)
        out_ref[part, :, mine] = own_ref[take]
        out_ref[part, :, other] = partner[take]


def fetch_tiles(source_hbm, target_ref, sems, tiles):
    tile = source_hbm.shape[0] // tiles
    loads = [
        pltpu.make_async_copy(
            source_hbm.at[pl.ds(index * tile, tile)],
            target_ref.at[pl.ds(index * tile, tile)],
            sems.at[index],
        )
        for index in range(tiles)
    ]
    for load in loads:
        load.start()
    return loads


def expert_kernel(rows_ref, gate_ref, up_ref, down_ref, out_hbm, stage_ref, sems):
    contract = (((1,), (1,)), ((), ()))

    def make(start, tile):
        rows = rows_ref[start : start + tile]
        gate = lax.dot_general(rows, gate_ref[...], contract, preferred_element_type=jnp.float32)
        up = lax.dot_general(rows, up_ref[...], contract, preferred_element_type=jnp.float32)
        hidden = (gate / (1.0 + jnp.exp(-gate)) * up).astype(jnp.bfloat16)
        return jnp.dot(hidden, down_ref[...], preferred_element_type=jnp.float32).astype(
            jnp.bfloat16
        )

    send_tiles(make, out_hbm, stage_ref, sems)


def combine_kernel(combine_ref, rows_hbm, out_ref, rows_ref, total_ref, sems):
    tiles = sems.shape[0]
    tile = rows_hbm.shape[0] // tiles
    for index, load in enumerate(fetch_tiles(rows_hbm, rows_ref, sems, tiles)):
        load.wait()
        take = slice(index * tile, (index + 1) * tile)
        product = jnp.dot(
            combine_ref[:, take], rows_ref[take], preferred_element_type=jnp.float32
        )
        if index == 0:
            total_ref[...] = product
        elif index < tiles - 1:
            total_ref[...] += product
        else:
            out_ref[...] = (total_ref[...] + product).astype(jnp.bfloat16)


def in_vmem():
    return pl.BlockSpec(memory_space=pltpu.VMEM)


def in_smem():
    return pl.BlockSpec(memory_space=pltpu.SMEM)


def a2a(value, axes):
    return lax.all_to_all(value, axes, split_axis=0, concat_axis=0, tiled=True)


def norm_kernel(pieces_ref, hidden_ref, gain_ref, routing_ref, resid_ref, out_ref, row_ref, sems):
    width = hidden_ref.shape[2]
    resid = hidden_ref[0].astype(jnp.float32)
    resid = resid + jnp.sum(pieces_ref[...].astype(jnp.float32), axis=0)
    resid_ref[...] = resid
    mean = jnp.mean(resid * resid, axis=1, keepdims=True)
    row_ref[:, :width] = (resid * lax.rsqrt(mean + 1e-06) * gain_ref[...]).astype(jnp.bfloat16)
    row_ref[:, width:] = routing_ref[...]
    copies = [
        pltpu.make_async_copy(row_ref, out_ref.at[peer], sems.at[peer])
        for peer in range(out_ref.shape[0])
    ]
    for copy in copies:
        copy.start()
    for copy in copies:
        copy.wait()


def routed(part_ref, gathered_ref):
    top_k, block = 8, 16
    rows, width = gathered_ref.shape[0], gathered_ref.shape[1] - 128
    columns = jnp.transpose(gathered_ref[:, width:].astype(jnp.float32))
    chosen = columns[:top_k]
    mixing = columns[top_k : 2 * top_k]
    sides, xs, ps, qs, zs = 2, 4, 4, 2, 2
    local = sides * xs * qs * zs
    place = lax.broadcasted_iota(jnp.int32, (local, rows), 0)
    at_z = (place // sides) % zs
    at_q = (place // (sides * zs)) % qs
    at_x = place // (sides * zs * qs)
    expert = (((place % sides) * xs + at_x) * (ps * qs) + part_ref[0] * qs + at_q) * zs + at_z
    expert = expert.astype(jnp.float32)
    named = jnp.zeros((local, rows), jnp.float32)
    weight = jnp.zeros((local, rows), jnp.float32)
    for k in range(top_k):
        hit = chosen[k : k + 1] == expert
        named = jnp.where(hit, 1.0, named)
        weight = jnp.where(hit, mixing[k : k + 1], weight)
    first = lax.broadcasted_iota(jnp.int32, (rows, rows), 0)
    second = lax.broadcasted_iota(jnp.int32, (rows, rows), 1)
    earlier = (first < second) & (first // block == second // block)
    rank = jnp.dot(
        named.astype(jnp.bfloat16),
        jnp.where(earlier, 1.0, 0.0).astype(jnp.bfloat16),
        preferred_element_type=jnp.float32,
    )
    blocks = rows // block
    own = lax.broadcasted_iota(jnp.int32, (blocks, rows), 0) == (
        lax.broadcasted_iota(jnp.int32, (blocks, rows), 1) // block
    )
    return named, rank, weight, own


def send_tiles(make, out_hbm, stage_ref, sems):
    slots, tile = stage_ref.shape[0], stage_ref.shape[1]
    copies = []
    for index in range(out_hbm.shape[0] // tile):
        slot = index % slots
        if index >= slots:
            copies[index - slots].wait()
        stage_ref[slot] = make(index * tile, tile)
        copy = pltpu.make_async_copy(
            stage_ref.at[slot], out_hbm.at[pl.ds(index * tile, tile)], sems.at[slot]
        )
        copy.start()
        copies.append(copy)
    for copy in copies[-slots:]:
        copy.wait()


def dispatch_kernel(part_ref, gathered_ref, out_ref, dispatch_ref):
    width = gathered_ref.shape[1] - 128
    named, rank, _, own = routed(part_ref, gathered_ref)
    blocks = own.shape[0]
    for e in range(named.shape[0]):
        for s in range(2):
            takes = (named[e : e + 1] > 0.5) & (jnp.abs(rank[e : e + 1] - s) < 0.5)
            at = (2 * e + s) * blocks
            dispatch_ref[at : at + blocks] = jnp.where(
                own, jnp.where(takes, 1.0, 0.0), 0.0
            ).astype(jnp.bfloat16)
    tile = 256

    def step(index, carry):
        take = pl.ds(pl.multiple_of(index * tile, tile), tile)
        out_ref[take, :] = jnp.dot(
            dispatch_ref[take, :], gathered_ref[:, :width], preferred_element_type=jnp.float32
        ).astype(jnp.bfloat16)
        return carry

    lax.fori_loop(0, out_ref.shape[0] // tile, step, 0)


def weight_kernel(part_ref, gathered_ref, combine_ref):
    named, rank, weight, own = routed(part_ref, gathered_ref)
    blocks = own.shape[0]
    group = 128 // (2 * blocks)
    for start in range(0, named.shape[0], group):
        tiles = []
        for e in range(start, start + group):
            for s in range(2):
                takes = (named[e : e + 1] > 0.5) & (jnp.abs(rank[e : e + 1] - s) < 0.5)
                tiles.append(jnp.where(own, jnp.where(takes, weight[e : e + 1], 0.0), 0.0))
        at = 2 * start * blocks
        combine_ref[:, at : at + 128] = jnp.transpose(jnp.concatenate(tiles, axis=0)).astype(
            jnp.bfloat16
        )


def shards(
    q_new,
    k_cache,
    value_cache,
    k_new,
    new_value_rows,
    cache_len,
    hidden_in,
    out_proj,
    norm_gain,
    expert_ids,
    gate_wts,
    w_gate,
    w_up,
    w_down,
):
    width = hidden_in.shape[2]
    block = hidden_in.shape[1]
    side = lax.axis_index("side")
    quarters = lax.axis_size("head")
    near = lax.axis_size(NEAR)
    far = lax.axis_size(FAR)
    slots = 2 * near

    partner_proj = lax.ppermute(out_proj, "side", [(0, 1), (1, 0)])
    half = out_proj.shape[1]
    rows_here = q_new.shape[1]
    context, own = pl.pallas_call(
        attention_kernel,
        in_specs=[in_smem()] + [pl.BlockSpec(memory_space=pltpu.HBM)] * 6,
        out_specs=[in_vmem()] * 2,
        scratch_shapes=[
            pltpu.VMEM(value.shape, jnp.bfloat16)
            for value in (q_new, k_cache, value_cache, k_new, new_value_rows, out_proj)
        ]
        + [pltpu.SemaphoreType.DMA((6,))],
        out_shape=[
            jax.ShapeDtypeStruct((rows_here, q_new.shape[2]), jnp.bfloat16),
            jax.ShapeDtypeStruct((rows_here, half), jnp.bfloat16),
        ],
        cost_estimate=pl.CostEstimate(
            flops=400_000_000, bytes_accessed=3_000_000, transcendentals=300_000
        ),
        compiler_params=pltpu.CompilerParams(vmem_limit_bytes=12 << 20),
        name="attention",
    )(
        cache_len,
        *(
            pltpu.with_memory_space_constraint(value, pltpu.HBM)
            for value in (q_new, k_cache, value_cache, k_new, new_value_rows, out_proj)
        ),
    )
    full_rows = pl.pallas_call(
        project_kernel,
        in_specs=[in_smem(), in_vmem(), pl.BlockSpec(memory_space=pl.ANY), in_vmem()],
        out_specs=in_vmem(),
        scratch_shapes=[pltpu.VMEM(out_proj.shape, jnp.bfloat16), pltpu.SemaphoreType.DMA],
        out_shape=jax.ShapeDtypeStruct((quarters, block, width), jnp.bfloat16),
        cost_estimate=pl.CostEstimate(
            flops=140_000_000, bytes_accessed=2_500_000, transcendentals=0
        ),
        compiler_params=pltpu.CompilerParams(vmem_limit_bytes=12 << 20),
        name="project",
    )(side.reshape(1), context, partner_proj, own)
    pieces = a2a(full_rows, "head")
    raw_wts = gate_wts[0]
    mixing = (raw_wts / jnp.sum(raw_wts, axis=-1, keepdims=True)).astype(jnp.bfloat16)
    routing = jnp.concatenate([expert_ids[0].astype(jnp.bfloat16), mixing], axis=1)
    routing = jnp.pad(routing, ((0, 0), (0, 128 - routing.shape[1])))
    resid, payload = pl.pallas_call(
        norm_kernel,
        in_specs=[in_vmem()] * 4,
        out_specs=[in_vmem(), pl.BlockSpec(memory_space=pltpu.HBM)],
        out_shape=[
            jax.ShapeDtypeStruct((block, width), jnp.float32),
            jax.ShapeDtypeStruct((near, block, width + 128), jnp.bfloat16),
        ],
        scratch_shapes=[
            pltpu.VMEM((block, width + 128), jnp.bfloat16),
            pltpu.SemaphoreType.DMA((near,)),
        ],
        cost_estimate=pl.CostEstimate(flops=500_000, bytes_accessed=1_500_000, transcendentals=0),
        compiler_params=pltpu.CompilerParams(vmem_limit_bytes=8 << 20),
        name="norm",
    )(pieces, hidden_in, norm_gain.reshape(1, width), routing)
    gathered = a2a(payload, NEAR)
    gathered = gathered.reshape(near * block, width + 128)
    part = lax.axis_index("yp").reshape(1)
    tile = 256
    outgoing = pl.pallas_call(
        dispatch_kernel,
        in_specs=[in_smem(), in_vmem()],
        out_specs=in_vmem(),
        out_shape=jax.ShapeDtypeStruct((far * slots, width), jnp.bfloat16),
        cost_estimate=pl.CostEstimate(
            flops=1_200_000_000, bytes_accessed=6_000_000, transcendentals=0
        ),
        scratch_shapes=[pltpu.VMEM((far * slots, near * block), jnp.bfloat16)],
        compiler_params=pltpu.CompilerParams(vmem_limit_bytes=20 << 20),
        name="dispatch",
    )(part, gathered)
    flat_rows = a2a(outgoing.reshape(far, slots, width), FAR).reshape(far * slots, width)
    partial_value = pl.pallas_call(
        expert_kernel,
        in_specs=[in_vmem()] * 4,
        out_specs=pl.BlockSpec(memory_space=pltpu.HBM),
        out_shape=pltpu.HBM((far * slots, width), jnp.bfloat16),
        scratch_shapes=[
            pltpu.VMEM((2, tile, width), jnp.bfloat16),
            pltpu.SemaphoreType.DMA((2,)),
        ],
        cost_estimate=pl.CostEstimate(
            flops=2_500_000_000, bytes_accessed=11_000_000, transcendentals=200_000
        ),
        compiler_params=pltpu.CompilerParams(vmem_limit_bytes=24 << 20),
        name="experts",
    )(flat_rows, w_gate[0].T, w_up[0].T, w_down[0])
    partial_value, gathered = lax.optimization_barrier((partial_value, gathered))
    combine = pl.pallas_call(
        weight_kernel,
        in_specs=[in_smem(), in_vmem()],
        out_specs=in_vmem(),
        out_shape=jax.ShapeDtypeStruct((near * block, far * slots), jnp.bfloat16),
        cost_estimate=pl.CostEstimate(
            flops=200_000_000, bytes_accessed=1_200_000, transcendentals=0
        ),
        compiler_params=pltpu.CompilerParams(vmem_limit_bytes=12 << 20),
        name="weights",
    )(part, gathered)
    returned = a2a(partial_value.reshape(far, slots, width), FAR).reshape(far * slots, width)
    weighted = pl.pallas_call(
        combine_kernel,
        in_specs=[in_vmem(), pl.BlockSpec(memory_space=pl.ANY)],
        out_specs=in_vmem(),
        scratch_shapes=[
            pltpu.VMEM((far * slots, width), jnp.bfloat16),
            pltpu.VMEM((near * block, width), jnp.float32),
            pltpu.SemaphoreType.DMA((far * slots // tile,)),
        ],
        out_shape=jax.ShapeDtypeStruct((near * block, width), jnp.bfloat16),
        cost_estimate=pl.CostEstimate(
            flops=1_100_000_000, bytes_accessed=6_000_000, transcendentals=0
        ),
        compiler_params=pltpu.CompilerParams(vmem_limit_bytes=16 << 20),
        name="combine",
    )(combine, returned)
    parts = a2a(weighted.reshape(near, block, width), NEAR)
    moe_out = jnp.sum(parts.astype(jnp.float32), axis=0)
    return (resid + moe_out).astype(jnp.bfloat16)[None]


def solution(mesh):
    fine = Mesh(
        mesh.devices.reshape(2, 4, 4, 2, 2, 4), ("side", "x", "yp", "yq", "zl", "head")
    )
    in_specs = (
        P(STREAM, None, "head"),
        P(STREAM, "head", None, None),
        P(STREAM, "head", None, None),
        P(STREAM, None, "head"),
        P(STREAM, None, "head"),
        P(STREAM),
        P(STREAM, "head", None),
        P("head", "side"),
        P(),
        P(STREAM, "head", None),
        P(STREAM, "head", None),
        P(STREAM, None, "head"),
        P(STREAM, None, "head"),
        P(STREAM, "head", None),
    )
    out_specs = P(STREAM, "head", None)
    return jax.shard_map(shards, mesh=fine, in_specs=in_specs, out_specs=out_specs, check_vma=False)
```

```python
import math

import jax
import jax.numpy as jnp
from jax import lax
from jax.experimental import pallas as pl
from jax.experimental.pallas import tpu as pltpu
from jax.sharding import Mesh
from jax.sharding import PartitionSpec as P

STREAM = ("side", "x", "yp", "yq", "zl")
NEAR = ("head", "yp")
FAR = ("x", "yq", "zl", "side")


def attention_kernel(
    len_ref,
    q_hbm,
    k_hbm,
    v_hbm,
    kn_hbm,
    vn_hbm,
    proj_hbm,
    ctx_ref,
    own_ref,
    q_ref,
    k_ref,
    v_ref,
    kn_ref,
    vn_ref,
    proj_ref,
    sems,
):
    pairs = (
        (q_hbm, q_ref),
        (k_hbm, k_ref),
        (kn_hbm, kn_ref),
        (v_hbm, v_ref),
        (vn_hbm, vn_ref),
        (proj_hbm, proj_ref),
    )
    loads = [
        pltpu.make_async_copy(source, target, sems.at[index])
        for index, (source, target) in enumerate(pairs)
    ]
    for load in loads:
        load.start()
    for load in loads[:-1]:
        load.wait()
    rows = q_ref.shape[1]
    cached, size = k_ref.shape[2], k_ref.shape[3]
    groups = q_ref.shape[2] // size
    per = 2
    scale = 1.0 / math.sqrt(size)
    old_key, new_key = k_ref[0, 0], kn_ref[0]
    old_val, new_val = v_ref[0, 0], vn_ref[0]
    contract = (((1,), (1,)), ((), ()))
    key_pos = lax.broadcasted_iota(jnp.int32, (per * rows, cached), 1)
    old_seen = key_pos < len_ref[0]
    row_pos = lax.broadcasted_iota(jnp.int32, (per * rows, rows), 0) % rows
    new_seen = lax.broadcasted_iota(jnp.int32, (per * rows, rows), 1) <= row_pos
    for start in range(0, groups, per):
        query = jnp.concatenate(
            [q_ref[0, :, (start + g) * size : (start + g + 1) * size] for g in range(per)], axis=0
        )
        old = lax.dot_general(query, old_key, contract, preferred_element_type=jnp.float32) * scale
        new = lax.dot_general(query, new_key, contract, preferred_element_type=jnp.float32) * scale
        old = jnp.where(old_seen, old, -jnp.inf)
        new = jnp.where(new_seen, new, -jnp.inf)
        highest = jnp.maximum(
            jnp.max(old, axis=1, keepdims=True), jnp.max(new, axis=1, keepdims=True)
        )
        old = jnp.exp(old - highest)
        new = jnp.exp(new - highest)
        total = jnp.sum(old, axis=1, keepdims=True) + jnp.sum(new, axis=1, keepdims=True)
        share = 1.0 / total
        context = jnp.dot(
            (old * share).astype(jnp.bfloat16), old_val, preferred_element_type=jnp.float32
        ) + jnp.dot((new * share).astype(jnp.bfloat16), new_val, preferred_element_type=jnp.float32)
        context = context.astype(jnp.bfloat16)
        for g in range(per):
            ctx_ref[:, (start + g) * size : (start + g + 1) * size] = context[
                g * rows : (g + 1) * rows
            ]
    loads[-1].wait()
    own_ref[...] = jnp.dot(
        ctx_ref[...], proj_ref[...], preferred_element_type=jnp.float32
    ).astype(jnp.bfloat16)


def project_kernel(side_ref, ctx_ref, proj_any, own_ref, out_ref, proj_ref, sem):
    load = pltpu.make_async_copy(proj_any, proj_ref, sem)
    load.start()
    load.wait()
    half = proj_ref.shape[1]
    block = out_ref.shape[1]
    side = side_ref[0]
    partner = jnp.dot(
        ctx_ref[...], proj_ref[...], preferred_element_type=jnp.float32
    ).astype(jnp.bfloat16)
    mine = pl.ds(pl.multiple_of(side * half, half), half)
    other = pl.ds(pl.multiple_of((1 - side) * half, half), half)
    for part in range(out_ref.shape[0]):
        take = slice(part * block, (part + 1) * block)
        out_ref[part, :, mine] = own_ref[take]
        out_ref[part, :, other] = partner[take]


def expert_kernel(rows_ref, gate_ref, up_ref, down_ref, out_ref):
    tile = 256
    contract = (((1,), (1,)), ((), ()))

    def step(index, carry):
        take = pl.ds(pl.multiple_of(index * tile, tile), tile)
        rows = rows_ref[take, :]
        gate = lax.dot_general(rows, gate_ref[...], contract, preferred_element_type=jnp.float32)
        up = lax.dot_general(rows, up_ref[...], contract, preferred_element_type=jnp.float32)
        hidden = (gate / (1.0 + jnp.exp(-gate)) * up).astype(jnp.bfloat16)
        out_ref[take, :] = jnp.dot(
            hidden, down_ref[...], preferred_element_type=jnp.float32
        ).astype(jnp.bfloat16)
        return carry

    lax.fori_loop(0, rows_ref.shape[0] // tile, step, 0, unroll=True)


def combine_kernel(combine_ref, rows_ref, out_ref):
    tile = 512

    def step(index, carry):
        take = pl.ds(pl.multiple_of(index * tile, tile), tile)
        out_ref[:, take] = jnp.dot(
            combine_ref[...], rows_ref[:, take], preferred_element_type=jnp.float32
        ).astype(jnp.bfloat16)
        return carry

    lax.fori_loop(0, rows_ref.shape[1] // tile, step, 0, unroll=True)


def in_vmem():
    return pl.BlockSpec(memory_space=pltpu.VMEM)


def in_smem():
    return pl.BlockSpec(memory_space=pltpu.SMEM)


def a2a(value, axes):
    return lax.all_to_all(value, axes, split_axis=0, concat_axis=0, tiled=True)


def norm_kernel(pieces_ref, hidden_ref, gain_ref, routing_ref, resid_ref, out_ref, row_ref, sems):
    width = hidden_ref.shape[2]
    resid = hidden_ref[0].astype(jnp.float32)
    resid = resid + jnp.sum(pieces_ref[...].astype(jnp.float32), axis=0)
    resid_ref[...] = resid
    mean = jnp.mean(resid * resid, axis=1, keepdims=True)
    row_ref[:, :width] = (resid * lax.rsqrt(mean + 1e-06) * gain_ref[...]).astype(jnp.bfloat16)
    row_ref[:, width:] = routing_ref[...]
    copies = [
        pltpu.make_async_copy(row_ref, out_ref.at[peer], sems.at[peer])
        for peer in range(out_ref.shape[0])
    ]
    for copy in copies:
        copy.start()
    for copy in copies:
        copy.wait()


def dispatch_kernel(part_ref, gathered_ref, out_ref, combine_ref, dispatch_ref):
    top_k, block = 8, 16
    rows, width = gathered_ref.shape[0], gathered_ref.shape[1] - 128
    blocks = rows // block
    columns = jnp.transpose(gathered_ref[:, width:].astype(jnp.float32))
    chosen = columns[:top_k]
    mixing = columns[top_k : 2 * top_k]
    sides, xs, ps, qs, zs = 2, 4, 4, 2, 2
    local = sides * xs * qs * zs
    place = lax.broadcasted_iota(jnp.int32, (local, rows), 0)
    at_z = (place // sides) % zs
    at_q = (place // (sides * zs)) % qs
    at_x = place // (sides * zs * qs)
    expert = (((place % sides) * xs + at_x) * (ps * qs) + part_ref[0] * qs + at_q) * zs + at_z
    expert = expert.astype(jnp.float32)
    named = jnp.zeros((local, rows), jnp.float32)
    weight = jnp.zeros((local, rows), jnp.float32)
    for k in range(top_k):
        hit = chosen[k : k + 1] == expert
        named = jnp.where(hit, 1.0, named)
        weight = jnp.where(hit, mixing[k : k + 1], weight)
    first = lax.broadcasted_iota(jnp.int32, (rows, rows), 0)
    second = lax.broadcasted_iota(jnp.int32, (rows, rows), 1)
    earlier = (first < second) & (first // block == second // block)
    rank = jnp.dot(
        named.astype(jnp.bfloat16),
        jnp.where(earlier, 1.0, 0.0).astype(jnp.bfloat16),
        preferred_element_type=jnp.float32,
    )
    own = lax.broadcasted_iota(jnp.int32, (blocks, rows), 0) == (
        lax.broadcasted_iota(jnp.int32, (blocks, rows), 1) // block
    )
    group = 128 // (2 * blocks)
    for start in range(0, local, group):
        tiles = []
        for e in range(start, start + group):
            for s in range(2):
                takes = (named[e : e + 1] > 0.5) & (jnp.abs(rank[e : e + 1] - s) < 0.5)
                at = (2 * e + s) * blocks
                dispatch_ref[at : at + blocks] = jnp.where(
                    own, jnp.where(takes, 1.0, 0.0), 0.0
                ).astype(jnp.bfloat16)
                tiles.append(jnp.where(own, jnp.where(takes, weight[e : e + 1], 0.0), 0.0))
        at = 2 * start * blocks
        turned = jnp.transpose(jnp.concatenate(tiles, axis=0)).astype(jnp.bfloat16)
        combine_ref[:, at : at + 128] = turned
    tile = 256

    def step(index, carry):
        take = pl.ds(pl.multiple_of(index * tile, tile), tile)
        out_ref[take, :] = jnp.dot(
            dispatch_ref[take, :], gathered_ref[:, :width], preferred_element_type=jnp.float32
        ).astype(jnp.bfloat16)
        return carry

    lax.fori_loop(0, out_ref.shape[0] // tile, step, 0, unroll=True)


def shards(
    q_new,
    k_cache,
    value_cache,
    k_new,
    new_value_rows,
    cache_len,
    hidden_in,
    out_proj,
    norm_gain,
    expert_ids,
    gate_wts,
    w_gate,
    w_up,
    w_down,
):
    width = hidden_in.shape[2]
    block = hidden_in.shape[1]
    side = lax.axis_index("side")
    quarters = lax.axis_size("head")
    near = lax.axis_size(NEAR)
    far = lax.axis_size(FAR)
    slots = 2 * near

    partner_proj = lax.ppermute(out_proj, "side", [(0, 1), (1, 0)])
    half = out_proj.shape[1]
    rows_here = q_new.shape[1]
    context, own = pl.pallas_call(
        attention_kernel,
        in_specs=[in_smem()] + [pl.BlockSpec(memory_space=pltpu.HBM)] * 6,
        out_specs=[in_vmem()] * 2,
        scratch_shapes=[
            pltpu.VMEM(value.shape, jnp.bfloat16)
            for value in (q_new, k_cache, value_cache, k_new, new_value_rows, out_proj)
        ]
        + [pltpu.SemaphoreType.DMA((6,))],
        out_shape=[
            jax.ShapeDtypeStruct((rows_here, q_new.shape[2]), jnp.bfloat16),
            jax.ShapeDtypeStruct((rows_here, half), jnp.bfloat16),
        ],
        cost_estimate=pl.CostEstimate(
            flops=400_000_000, bytes_accessed=3_000_000, transcendentals=300_000
        ),
        compiler_params=pltpu.CompilerParams(vmem_limit_bytes=12 << 20),
        name="attention",
    )(
        cache_len,
        *(
            pltpu.with_memory_space_constraint(value, pltpu.HBM)
            for value in (q_new, k_cache, value_cache, k_new, new_value_rows, out_proj)
        ),
    )
    full_rows = pl.pallas_call(
        project_kernel,
        in_specs=[in_smem(), in_vmem(), pl.BlockSpec(memory_space=pl.ANY), in_vmem()],
        out_specs=in_vmem(),
        scratch_shapes=[pltpu.VMEM(out_proj.shape, jnp.bfloat16), pltpu.SemaphoreType.DMA],
        out_shape=jax.ShapeDtypeStruct((quarters, block, width), jnp.bfloat16),
        cost_estimate=pl.CostEstimate(
            flops=140_000_000, bytes_accessed=2_500_000, transcendentals=0
        ),
        compiler_params=pltpu.CompilerParams(vmem_limit_bytes=12 << 20),
        name="project",
    )(side.reshape(1), context, partner_proj, own)
    pieces = a2a(full_rows, "head")
    raw_wts = gate_wts[0]
    mixing = (raw_wts / jnp.sum(raw_wts, axis=-1, keepdims=True)).astype(jnp.bfloat16)
    routing = jnp.concatenate([expert_ids[0].astype(jnp.bfloat16), mixing], axis=1)
    routing = jnp.pad(routing, ((0, 0), (0, 128 - routing.shape[1])))
    resid, payload = pl.pallas_call(
        norm_kernel,
        in_specs=[in_vmem()] * 4,
        out_specs=[in_vmem(), pl.BlockSpec(memory_space=pltpu.HBM)],
        out_shape=[
            jax.ShapeDtypeStruct((block, width), jnp.float32),
            jax.ShapeDtypeStruct((near, block, width + 128), jnp.bfloat16),
        ],
        scratch_shapes=[
            pltpu.VMEM((block, width + 128), jnp.bfloat16),
            pltpu.SemaphoreType.DMA((near,)),
        ],
        cost_estimate=pl.CostEstimate(flops=500_000, bytes_accessed=1_500_000, transcendentals=0),
        compiler_params=pltpu.CompilerParams(vmem_limit_bytes=8 << 20),
        name="norm",
    )(pieces, hidden_in, norm_gain.reshape(1, width), routing)
    gathered = a2a(payload, NEAR)
    outgoing, combine = pl.pallas_call(
        dispatch_kernel,
        in_specs=[in_smem(), in_vmem()],
        out_specs=[in_vmem()] * 2,
        out_shape=[
            jax.ShapeDtypeStruct((far * slots, width), jnp.bfloat16),
            jax.ShapeDtypeStruct((near * block, far * slots), jnp.bfloat16),
        ],
        cost_estimate=pl.CostEstimate(
            flops=1_200_000_000, bytes_accessed=6_000_000, transcendentals=0
        ),
        scratch_shapes=[pltpu.VMEM((far * slots, near * block), jnp.bfloat16)],
        compiler_params=pltpu.CompilerParams(vmem_limit_bytes=20 << 20),
        name="dispatch",
    )(lax.axis_index("yp").reshape(1), gathered.reshape(near * block, width + 128))

    flat_rows = a2a(outgoing.reshape(far, slots, width), FAR).reshape(far * slots, width)
    partial_value = pl.pallas_call(
        expert_kernel,
        in_specs=[in_vmem()] * 4,
        out_specs=in_vmem(),
        out_shape=jax.ShapeDtypeStruct((far * slots, width), jnp.bfloat16),
        cost_estimate=pl.CostEstimate(
            flops=2_500_000_000, bytes_accessed=11_000_000, transcendentals=200_000
        ),
        compiler_params=pltpu.CompilerParams(vmem_limit_bytes=24 << 20),
        name="experts",
    )(flat_rows, w_gate[0].T, w_up[0].T, w_down[0])
    returned = a2a(partial_value.reshape(far, slots, width), FAR).reshape(far * slots, width)
    weighted = pl.pallas_call(
        combine_kernel,
        in_specs=[in_vmem()] * 2,
        out_specs=in_vmem(),
        out_shape=jax.ShapeDtypeStruct((near * block, width), jnp.bfloat16),
        cost_estimate=pl.CostEstimate(
            flops=1_100_000_000, bytes_accessed=6_000_000, transcendentals=0
        ),
        compiler_params=pltpu.CompilerParams(vmem_limit_bytes=16 << 20),
        name="combine",
    )(combine, returned)
    parts = a2a(weighted.reshape(near, block, width), NEAR)
    moe_out = jnp.sum(parts.astype(jnp.float32), axis=0)
    return (resid + moe_out).astype(jnp.bfloat16)[None]


def solution(mesh):
    fine = Mesh(
        mesh.devices.reshape(2, 4, 4, 2, 2, 4), ("side", "x", "yp", "yq", "zl", "head")
    )
    in_specs = (
        P(STREAM, None, "head"),
        P(STREAM, "head", None, None),
        P(STREAM, "head", None, None),
        P(STREAM, None, "head"),
        P(STREAM, None, "head"),
        P(STREAM),
        P(STREAM, "head", None),
        P("head", "side"),
        P(),
        P(STREAM, "head", None),
        P(STREAM, "head", None),
        P(STREAM, None, "head"),
        P(STREAM, None, "head"),
        P(STREAM, "head", None),
    )
    out_specs = P(STREAM, "head", None)
    return jax.shard_map(shards, mesh=fine, in_specs=in_specs, out_specs=out_specs, check_vma=False)
```
